128 devices in a mesh: sub: 8 (over x, core), lat: 8 (over y_lo, z), lon: 2 (over y_hi).
Axes of the slice: x: 4, y: 4 (y_hi: 2, y_lo: 2; y = y_hi * 2 + y_lo), z: 4, core: 2. Of those that a mesh axis runs over, the one named last changes fastest.
Arguments:
- increment: float32 [8, 128, 128, 512], P('sub', 'lat', 'lon'), may hold values from -6 to 6
- multiplier: float32 [8, 128, 128, 512], P('sub', 'lat', 'lon'), may hold values from -6 to 6
- background: bfloat16 [8, 128, 128, 512], P('sub', 'lat', 'lon'), may hold values from -6 to 6
- obs_cotangent: bfloat16 [8, 16, 2048, 512], P('sub', ('lat', 'lon')), may hold values from -6 to 6
- obs_column: int32 [8, 16, 2048], P('sub', ('lat', 'lon')), may hold values from 0 to 1023
- obs_count: int32 [8, 16], P('sub'), may hold values from 1 to 2048, 16384 in all within a row
- transport: float32 [8, 512], replicated, may hold values from 0.015 to 0.1
- hidden_weight: bfloat16 [512, 1024], replicated, may hold values from -0.25 to 0.25
- hidden_bias: float32 [1024], replicated, may hold values from -3 to 3
- output_weight: bfloat16 [1024, 512], replicated, may hold values from -0.1875 to 0.1875
Outputs:
- model_error: float32 [8, 128, 128, 512], P('sub', 'lat', 'lon')
- gradient: float32 [8, 128, 128, 512], P('sub', 'lat', 'lon')
- obs_tangent: bfloat16 [8, 16, 2048, 512], P('sub', ('lat', 'lon'))
The draws below stay inside these ranges and needn't reach their ends.
Inputs may be any that keep to these rules, and one draw needn't show every extreme that they name: `obs_count`: the counts of one subwindow sum to 16384, and one of them equals 2048. `obs_column`: slots at or beyond their block's count are unused.
All inputs are finite; a program needn't handle non-finite values.
Results may differ from the reference program's by a relative error of at most 0.0058.
Values may be sent and summed in bfloat16 or wider, within the bound.
No kernel may reach another device: no remote copies, remote signals or barrier semaphores. Data moves between devices by JAX's collectives and lax.ppermute only.
A program may use at most 128 MiB of HBM per device.

```python
import math
import jax
import jax.numpy as jnp
import numpy as np
from jax import lax

LEV = 512
HID = 1024
CHAN = 512
LAT_DEV = 16
LON_DEV = 64
OBS_DEV = 2048
STEPS = 4
SUBS = 8
NLAT = 128
NLON = 128
OWNERS = 16
COLS = 1024
N_LAT = 8
N_LON = 2


def plant(entries, key, least, largest):
    spot = [jax.random.randint(jax.random.fold_in(key, axis), (), 0, length) for axis, length in enumerate(entries.shape)]
    main_axis = entries.shape.index(max(entries.shape))
    neighbour = spot[:main_axis] + [(spot[main_axis] + 1) % entries.shape[main_axis]] + spot[main_axis + 1:]
    return entries.at[tuple(spot)].set(least).at[tuple(neighbour)].set(largest)


def level_of(own_key, shape, pieces, low, high):
    def one(dim, parts):
        draws = jax.random.uniform(jax.random.fold_in(jax.random.fold_in(own_key, 6), dim), (parts,), jnp.float32, low / len(pieces), high / len(pieces))
        return jnp.repeat(jnp.exp(draws), shape[dim] // parts).reshape((-1,) + (1,) * (len(shape) - dim - 1))

    factor_of = one(*pieces[0])
    for cut in pieces[1:]:
        factor_of = factor_of * one(*cut)
    return factor_of


def profile(amount, total, limit, slope):
    weights = [(1 << 20) // math.isqrt(grade ** slope) + 1 for grade in range(2, amount + 1)]
    spare, counts = total - limit - (amount - 1), [1] * (amount - 1)
    while spare > 0:
        movable = [i for i in range(amount - 1) if counts[i] < limit]
        pool, budget = sum([weights[i] for i in movable]), spare
        for i in movable:
            extra = min(limit - counts[i], max(1, budget * weights[i] // pool), spare)
            counts[i] = counts[i] + extra
            spare = spare - extra
    return np.array([limit] + counts)


def ragged_sizes(key, number_of, total, most, slope):
    if number_of == 2:
        one = jax.random.randint(key, (), max(1, total - most), min(most, total - 1) + 1)
        return jnp.stack([one, total - one])
    tallies = jnp.asarray(profile(number_of, total, most, slope), jnp.int32)
    pairs = (number_of - 1) // 2
    donor, taker = tallies[1:1 + 2 * pairs:2], tallies[2:2 + 2 * pairs:2]
    margin = jnp.minimum(donor - 1, most - taker)
    passed = jax.random.randint(jax.random.fold_in(key, 1), (pairs,), 0, 1 << 20) % (margin + 1)
    tallies = tallies.at[1:1 + 2 * pairs:2].set(donor - passed).at[2:2 + 2 * pairs:2].set(taker + passed)
    return tallies[jax.random.permutation(jax.random.fold_in(key, 2), number_of)]


def noise(key, extent, scale, most, shards=(), kind=jnp.bfloat16):
    values = scale * jax.random.normal(key, extent, jnp.float32)
    if shards:
        values = values * level_of(key, extent, shards, -0.22, 0.18)
    return jnp.clip(values, -most, most).astype(kind)


def setup_inputs(seed: int = 0) -> dict:
    key_list = jax.random.split(jax.random.key(seed), 11)
    increment = noise(key_list[0], (SUBS, NLAT, NLON, LEV), 1.0, 6.0, ((0, 8), (1, 8), (2, 2)), jnp.float32)
    multiplier = noise(key_list[1], (SUBS, NLAT, NLON, LEV), 1.0, 6.0, ((0, 8), (1, 8), (2, 2)), jnp.float32)
    background = noise(key_list[2], (SUBS, NLAT, NLON, LEV), 1.0, 6.0, ((0, 8), (1, 8), (2, 2)))
    obs_cotangent = noise(key_list[3], (SUBS, OWNERS, OBS_DEV, CHAN), 1.0, 6.0, ((0, 8), (1, 16)))
    obs_column = plant(jax.random.randint(key_list[4], (SUBS, OWNERS, OBS_DEV), 0, COLS), jax.random.fold_in(key_list[4], 1), 0, COLS - 1).astype(jnp.int32)
    obs_count = jax.vmap(lambda own: ragged_sizes(own, OWNERS, OWNERS * OBS_DEV // 2, OBS_DEV, 2))(jax.random.split(key_list[5], SUBS)).reshape((SUBS, OWNERS)).astype(jnp.int32)
    transport = jnp.clip(jnp.exp(jax.random.uniform(key_list[6], (8, LEV), jnp.float32, math.log(0.015), math.log(0.1))), 0.015, 0.1)
    hidden_weight = noise(key_list[7], (LEV, HID), LEV ** -0.5, 0.25)
    hidden_bias = noise(key_list[8], (HID,), 0.5, 3.0, (), jnp.float32)
    output_weight = noise(key_list[9], (HID, CHAN), HID ** -0.5, 0.1875)
    return dict(increment=increment, multiplier=multiplier, background=background, obs_cotangent=obs_cotangent, obs_column=obs_column, obs_count=obs_count, transport=transport, hidden_weight=hidden_weight, hidden_bias=hidden_bias, output_weight=output_weight)


def observe(state_rows, back_rows, cot_rows, hidden_weight, hidden_bias, output_weight):
    preact = jnp.dot(back_rows, hidden_weight, preferred_element_type=jnp.float32) + hidden_bias
    hidden = jnp.tanh(preact)
    slopes = 1.0 - hidden * hidden
    forward = jnp.dot(state_rows, hidden_weight, preferred_element_type=jnp.float32)
    scaled = (slopes * forward).astype(jnp.bfloat16)
    tangent = jnp.dot(scaled, output_weight, preferred_element_type=jnp.float32).astype(jnp.bfloat16)
    pulled = jnp.dot(cot_rows, output_weight.T, preferred_element_type=jnp.float32)
    weighted = (slopes * pulled).astype(jnp.bfloat16)
    adjoint = jnp.dot(weighted, hidden_weight.T, preferred_element_type=jnp.float32).astype(jnp.bfloat16)
    return tangent, adjoint


def mirrored(transport):
    return jnp.stack([transport[3], transport[2], transport[1], transport[0],
                      transport[7], transport[6], transport[5], transport[4]])


def advance(window, coeffs):
    total_rate = jnp.sum(coeffs, axis=0)
    height = window.shape[0]
    across = window.shape[1]
    for sweep_step in range(STEPS):
        padded = jnp.pad(window, ((2, 2), (2, 2), (0, 0)))
        window = ((1.0 - total_rate) * window
                  + coeffs[0] * padded[0:height, 2:across + 2]
                  + coeffs[1] * padded[1:height + 1, 2:across + 2]
                  + coeffs[2] * padded[3:height + 3, 2:across + 2]
                  + coeffs[3] * padded[4:height + 4, 2:across + 2]
                  + coeffs[4] * padded[2:height + 2, 0:across]
                  + coeffs[5] * padded[2:height + 2, 1:across + 1]
                  + coeffs[6] * padded[2:height + 2, 3:across + 3]
                  + coeffs[7] * padded[2:height + 2, 4:across + 4])
    return window


def to_blocks(full_field):
    shaped = full_field.reshape(SUBS, N_LAT, LAT_DEV, N_LON, LON_DEV, full_field.shape[-1])
    return shaped.transpose(0, 1, 3, 2, 4, 5).reshape(SUBS * OWNERS, COLS, full_field.shape[-1])


def reference(increment, multiplier, background, obs_cotangent, obs_column, obs_count, transport, hidden_weight, hidden_bias, output_weight):
    reverse_rates = mirrored(transport)
    ahead = lax.map(lambda window: advance(window, transport), increment)
    behind = lax.map(lambda window: advance(window, reverse_rates), multiplier)
    zero_slab = jnp.zeros_like(increment[0:1])
    model_error = increment - jnp.concatenate([zero_slab, ahead[:-1]], axis=0)
    state_blocks = to_blocks(increment)
    back_blocks = to_blocks(background)
    flat_columns = obs_column.reshape(SUBS * OWNERS, OBS_DEV)
    flat_cot = obs_cotangent.reshape(SUBS * OWNERS, OBS_DEV, CHAN)
    flat_count = obs_count.reshape(SUBS * OWNERS)

    def one_block(inputs):
        state_block, back_block, columns, cot_rows, slot_count = inputs
        alive_rows = (jnp.arange(OBS_DEV, dtype=jnp.int32) < slot_count)[:, None]
        tangent, adjoint = observe(state_block[columns].astype(jnp.bfloat16), back_block[columns], cot_rows,
                                   hidden_weight, hidden_bias, output_weight)
        tangent = jnp.where(alive_rows, tangent, jnp.zeros_like(tangent))
        adjoint_wide = jnp.where(alive_rows, adjoint.astype(jnp.float32), jnp.zeros((), jnp.float32))
        summed = jnp.zeros((COLS, LEV), jnp.float32).at[columns].add(adjoint_wide)
        return tangent, summed

    tangents, sums = lax.map(one_block, (state_blocks, back_blocks, flat_columns, flat_cot, flat_count))
    obs_tangent = tangents.reshape(SUBS, OWNERS, OBS_DEV, CHAN)
    obs_adjoint = sums.reshape(SUBS, N_LAT, N_LON, LAT_DEV, LON_DEV, LEV).transpose(0, 1, 3, 2, 4, 5).reshape(SUBS, NLAT, NLON, LEV)
    gradient = multiplier - jnp.concatenate([behind[1:], zero_slab], axis=0) + obs_adjoint
    return model_error, gradient, obs_tangent
```

```python
import functools

import jax
import jax.numpy as jnp
from jax import lax
from jax.experimental import pallas as pl
from jax.experimental.pallas import tpu as pltpu
from jax.sharding import PartitionSpec as P

STEPS = 4
REACH = 2 * STEPS
EDGE = REACH - 2
LANES = 128
COLS_TILE = 256
SLOTS_TILE = 512
MIRROR = (3, 2, 1, 0, 7, 6, 5, 4)


def pack_kernel(*refs):
    n_fields = 2
    ins, outs = refs[:n_fields], refs[n_fields:]
    lon = lax.axis_index("lon")
    rows, across = ins[0].shape[0], ins[0].shape[1]
    side = pl.multiple_of((across - REACH) * (1 - lon), REACH)
    for f in range(n_fields):
        src = ins[f]
        whole, low, high, strip, low_corner, high_corner = outs[6 * f : 6 * f + 6]
        for r in range(rows):
            row = src[r].astype(jnp.bfloat16)
            whole[r] = row
            if r < REACH:
                low[r] = row
            if r >= rows - REACH:
                high[r - rows + REACH] = row
            edge = src[r, pl.ds(side, REACH), :].astype(jnp.bfloat16)
            strip[r] = edge
            if r < EDGE:
                low_corner[r] = edge
            if r >= rows - EDGE:
                high_corner[r - rows + EDGE] = edge


def pack(increment, multiplier):
    rows, across, levels = increment.shape
    tile = lambda *shape: pl.BlockSpec(shape + (LANES,), lambda l: (0, 0, l))
    shapes = [(rows, across), (REACH, across), (REACH, across), (rows, REACH), (EDGE, REACH), (EDGE, REACH)] * 2
    return pl.pallas_call(
        pack_kernel,
        grid=(levels // LANES,),
        in_specs=[tile(rows, across)] * 2,
        out_specs=[tile(*s) for s in shapes],
        out_shape=[jax.ShapeDtypeStruct(s + (levels,), jnp.bfloat16) for s in shapes],
        name="pack",
    )(increment, multiplier)


def sweep(src, dst, taps, first, last, blocks):
    center, c0, c1, c2, c3, c4, c5, c6, c7 = taps
    group = 4

    def rows_of(it, carry):
        i = first + it * group
        for b in range(blocks):
            j = 8 + 8 * b
            at = [src[i - 2 + r, j : j + 8, :] for r in range(group + 4)]
            for r in range(group):
                total = center * at[r + 2] + c0 * at[r]
                total = total + c1 * at[r + 1]
                total = total + c2 * at[r + 3]
                total = total + c3 * at[r + 4]
                total = total + c4 * src[i + r, j - 2 : j + 6, :]
                total = total + c5 * src[i + r, j - 1 : j + 7, :]
                total = total + c6 * src[i + r, j + 1 : j + 9, :]
                total = total + c7 * src[i + r, j + 2 : j + 10, :]
                dst[i + r, j : j + 8, :] = total
        return carry

    lax.fori_loop(0, (last - first) // group, rows_of, 0)


def transport_kernel(*refs):
    fields = [refs[0:6], refs[6:12]]
    rates, inc, mul, obs = refs[12:16]
    error_out, grad_out = refs[16:18]
    bufs = refs[18:20]
    lat, lon = lax.axis_index("lat"), lax.axis_index("lon")
    n_lat = lax.axis_size("lat")
    rows, across = inc.shape[0], inc.shape[1]
    tall = rows + 2 * REACH
    blocks = (across + REACH) // 8
    own = pl.multiple_of(8 + REACH * lon, 8)
    beside = pl.multiple_of(8 + across * (1 - lon), 8)

    @pl.when(pl.program_id(0) == 0)
    def _():
        for buf in bufs:
            for r in range(tall):
                buf[r] = jnp.zeros(buf.shape[1:], jnp.float32)

    for f in range(2):
        whole, above, below, strip, above_corner, below_corner = fields[f]
        a, b = bufs
        for r in range(REACH):
            a[r, pl.ds(own, across), :] = above[r].astype(jnp.float32)
            a[rows + REACH + r, pl.ds(own, across), :] = below[r].astype(jnp.float32)
        for r in range(rows):
            a[REACH + r, pl.ds(own, across), :] = whole[r].astype(jnp.float32)
            a[REACH + r, pl.ds(beside, REACH), :] = strip[r].astype(jnp.float32)
        for r in range(EDGE):
            a[REACH - EDGE + r, pl.ds(beside, REACH), :] = above_corner[r].astype(jnp.float32)
            a[rows + REACH + r, pl.ds(beside, REACH), :] = below_corner[r].astype(jnp.float32)

        order = range(8) if f == 0 else MIRROR
        spread = [jnp.broadcast_to(rates[k : k + 1, :], (8, LANES)) for k in order]
        rest = spread[0]
        for k in range(1, 8):
            rest = rest + spread[k]
        taps = [1.0 - rest] + spread

        for t in range(STEPS):
            first, last = 2 * (t + 1), tall - 2 * (t + 1)
            sweep(a, b, taps, first, last, blocks)
            if t < STEPS - 1:
                zero = jnp.zeros(a.shape[1:], jnp.float32)

                @pl.when(lat == 0)
                def _(b=b, first=first, zero=zero):
                    for r in range(first, REACH):
                        b[r] = zero

                @pl.when(lat == n_lat - 1)
                def _(b=b, last=last, zero=zero):
                    for r in range(rows + REACH, last):
                        b[r] = zero

            a, b = b, a

        for r in range(rows):
            moved = a[REACH + r, pl.ds(own, across), :]
            if f == 0:
                error_out[r] = inc[r] - moved
            else:
                grad_out[r] = mul[r] - moved + obs[r]


def transported(pieces, rates, increment, multiplier, obs_adjoint):
    rows, across, levels = increment.shape
    tile = lambda a: pl.BlockSpec(a.shape[:-1] + (LANES,), lambda l, n=a.ndim: (0,) * (n - 1) + (l,))
    operands = (*pieces, rates, increment, multiplier, obs_adjoint)
    return pl.pallas_call(
        transport_kernel,
        grid=(levels // LANES,),
        in_specs=[tile(a) for a in operands],
        out_specs=[tile(increment)] * 2,
        out_shape=[jax.ShapeDtypeStruct(increment.shape, jnp.float32)] * 2,
        scratch_shapes=[pltpu.VMEM((rows + 2 * REACH, across + REACH + 16, LANES), jnp.float32)] * 2,
        cost_estimate=pl.CostEstimate(flops=100_000_000, bytes_accessed=13 << 20, transcendentals=0),
        name="transport",
    )(*operands)


ROWS_BY_COLS = (((1,), (1,)), ((), ()))


def network_kernel(
    count, columns, state, back, cot, hidden_weight, hidden_bias, output_weight,
    tangent_out, adjoint_out, tangents, column_of, slot_of,
):
    step = pl.program_id(0)
    slots = cot.shape[0]
    col_steps = tangents.shape[0] // COLS_TILE

    @pl.when(step == 0)
    def _():
        alive = lax.broadcasted_iota(jnp.int32, (1, slots), 1) < count[0]
        named = jnp.where(alive, columns[...], -1)
        column_of[...] = jnp.broadcast_to(named, column_of.shape)
        for s in range(0, slots, LANES):
            piece = jnp.broadcast_to(named[:, s : s + LANES], (LANES, LANES))
            slot_of[s : s + LANES, :] = piece.T

    @pl.when(step < col_steps)
    def _():
        preact = jnp.dot(back[...], hidden_weight[...], preferred_element_type=jnp.float32) + hidden_bias[...]
        hidden = jnp.tanh(preact)
        slopes = 1.0 - hidden * hidden
        forward = jnp.dot(
            state[...].astype(jnp.bfloat16), hidden_weight[...], preferred_element_type=jnp.float32
        )
        scaled = (slopes * forward).astype(jnp.bfloat16)
        tangent = jnp.dot(scaled, output_weight[...], preferred_element_type=jnp.float32)
        start = pl.multiple_of(step * COLS_TILE, COLS_TILE)
        tangents[pl.ds(start, COLS_TILE), :] = tangent.astype(jnp.bfloat16)
        ids = lax.broadcasted_iota(jnp.int32, (COLS_TILE, slots), 0) + start
        picks = jnp.where(column_of[0:1, :] == ids, 1.0, 0.0).astype(jnp.bfloat16)
        gathered = jnp.dot(picks, cot[...], preferred_element_type=jnp.float32).astype(jnp.bfloat16)
        pulled = lax.dot_general(gathered, output_weight[...], ROWS_BY_COLS, preferred_element_type=jnp.float32)
        weighted = (slopes * pulled).astype(jnp.bfloat16)
        adjoint_out[...] = lax.dot_general(
            weighted, hidden_weight[...], ROWS_BY_COLS, preferred_element_type=jnp.float32
        )

    @pl.when(step >= col_steps)
    def _():
        start = pl.multiple_of((step - col_steps) * SLOTS_TILE, SLOTS_TILE)
        mine = slot_of[pl.ds(start, SLOTS_TILE), :]
        lane = lax.broadcasted_iota(jnp.int32, mine.shape, 1)
        picks = jnp.concatenate(
            [
                jnp.where(mine == lane + k, 1.0, 0.0).astype(jnp.bfloat16)
                for k in range(0, tangents.shape[0], LANES)
            ],
            axis=1,
        )
        tangent_out[...] = jnp.dot(picks, tangents[...], preferred_element_type=jnp.float32).astype(jnp.bfloat16)


def network(count, columns, state, back, cot, hidden_weight, hidden_bias, output_weight):
    cols, levels = state.shape
    slots, chan = cot.shape
    col_steps, slot_steps = cols // COLS_TILE, slots // SLOTS_TILE
    whole = lambda a: pl.BlockSpec(a.shape, lambda i: (0, 0))
    by_cols = lambda width: pl.BlockSpec((COLS_TILE, width), lambda i: (jnp.minimum(i, col_steps - 1), 0))
    units = 5 * cols + 2 * slots
    return pl.pallas_call(
        network_kernel,
        grid=(col_steps + slot_steps,),
        in_specs=[
            pl.BlockSpec(memory_space=pltpu.SMEM),
            whole(columns),
            by_cols(levels),
            by_cols(levels),
            whole(cot),
            whole(hidden_weight),
            whole(hidden_bias),
            whole(output_weight),
        ],
        out_specs=[
            pl.BlockSpec((SLOTS_TILE, chan), lambda i: (jnp.maximum(i - col_steps, 0), 0)),
            by_cols(levels),
        ],
        out_shape=[
            jax.ShapeDtypeStruct((slots, chan), jnp.bfloat16),
            jax.ShapeDtypeStruct((cols, levels), jnp.float32),
        ],
        scratch_shapes=[
            pltpu.VMEM((cols, chan), jnp.bfloat16),
            pltpu.VMEM((8, slots), jnp.int32),
            pltpu.VMEM((slots, LANES), jnp.int32),
        ],
        cost_estimate=pl.CostEstimate(
            flops=2 * units * levels * hidden_bias.shape[1], bytes_accessed=12 << 20, transcendentals=1 << 20
        ),
        name="network",
    )(count, columns, state, back, cot, hidden_weight, hidden_bias, output_weight)


def sent(array, by_sub, by_lat, across):
    counts = [lax.axis_size(axis) for axis in ("sub", "lat", "lon")]
    pairs = []
    for s in range(counts[0]):
        for a in range(counts[1]):
            for o in range(counts[2]):
                to_s, to_a, to_o = s + by_sub, a + by_lat, (1 - o if across else o)
                if 0 <= to_s < counts[0] and 0 <= to_a < counts[1]:
                    pairs.append(
                        (
                            (s * counts[1] + a) * counts[2] + o,
                            (to_s * counts[1] + to_a) * counts[2] + to_o,
                        )
                    )
    return lax.ppermute(array, ("sub", "lat", "lon"), pairs)


def local(
    increment,
    multiplier,
    background,
    obs_cotangent,
    obs_column,
    obs_count,
    transport,
    hidden_weight,
    hidden_bias,
    output_weight,
):
    increment, multiplier = increment[0], multiplier[0]
    levels = increment.shape[2]
    packed = pack(increment, multiplier)
    pieces = []
    for f, by_sub in enumerate((1, -1)):
        whole, low, high, strip, low_corner, high_corner = packed[6 * f : 6 * f + 6]
        pieces += [
            sent(whole, by_sub, 0, False),
            sent(high, by_sub, 1, False),
            sent(low, by_sub, -1, False),
            sent(strip, by_sub, 0, True),
            sent(high_corner, by_sub, 1, True),
            sent(low_corner, by_sub, -1, True),
        ]
    myself = lax.axis_index(("lat", "lon"))
    my_count = lax.dynamic_slice(obs_count[0], (myself,), (1,))
    tangent, obs_adjoint = network(
        my_count,
        obs_column[0],
        increment.reshape(-1, levels),
        background[0].reshape(-1, levels),
        obs_cotangent[0, 0],
        hidden_weight,
        hidden_bias[None, :],
        output_weight,
    )
    model_error, gradient = transported(
        pieces, transport, increment, multiplier, obs_adjoint.reshape(increment.shape)
    )
    return (model_error[None], gradient[None], tangent[None, None])


def solution(mesh):
    in_specs = (
        P("sub", "lat", "lon", None),
        P("sub", "lat", "lon", None),
        P("sub", "lat", "lon", None),
        P("sub", ("lat", "lon"), None, None),
        P("sub", ("lat", "lon"), None),
        P("sub", None),
        P(),
        P(),
        P(),
        P(),
    )
    out_specs = (
        P("sub", "lat", "lon", None),
        P("sub", "lat", "lon", None),
        P("sub", ("lat", "lon"), None, None),
    )
    return jax.shard_map(local, mesh=mesh, in_specs=in_specs, out_specs=out_specs, check_vma=False)
```

```python
import functools

import jax
import jax.numpy as jnp
from jax import lax
from jax.experimental import pallas as pl
from jax.experimental.pallas import tpu as pltpu
from jax.sharding import PartitionSpec as P

STEPS = 4
REACH = 2 * STEPS
EDGE = REACH - 2
LANES = 128
COLS_TILE = 256
SLOTS_TILE = 512
MIRROR = (3, 2, 1, 0, 7, 6, 5, 4)


CHUNK = 4


def pack_kernel(inc, mul, low, high, strip, low_corner, high_corner, held, sems):
    lon = lax.axis_index("lon")
    rows, across = inc.shape[0], inc.shape[1]
    side = pl.multiple_of((across - REACH) * (1 - lon), REACH)
    copies = {}
    for start in range(0, rows, CHUNK):
        for f, src in enumerate((inc, mul)):
            part = pl.ds(start, CHUNK)
            copies[f, start] = pltpu.make_async_copy(src.at[part], held.at[f, part], sems.at[f, start // CHUNK])
            copies[f, start].start()
    for start in range(0, rows, CHUNK):
        for f in range(2):
            copies[f, start].wait()
            for r in range(start, start + CHUNK):
                row = held[f, r].astype(jnp.bfloat16)
                if r < REACH:
                    low[f, r] = row
                if r >= rows - REACH:
                    high[f, r - rows + REACH] = row
                edge = held[f, r, pl.ds(side, REACH), :].astype(jnp.bfloat16)
                strip[f, r] = edge
                if r < EDGE:
                    low_corner[f, r] = edge
                if r >= rows - EDGE:
                    high_corner[f, r - rows + EDGE] = edge


def by_lanes(a):
    return pl.BlockSpec(a.shape[:-1] + (LANES,), lambda l, n=a.ndim: (0,) * (n - 1) + (l,))


def pack(increment, multiplier):
    rows, across, levels = increment.shape
    shapes = [(2, REACH, across), (2, REACH, across), (2, rows, REACH), (2, EDGE, REACH), (2, EDGE, REACH)]
    outs = [jax.ShapeDtypeStruct(s + (levels,), jnp.bfloat16) for s in shapes]
    return pl.pallas_call(
        pack_kernel,
        in_specs=[pl.BlockSpec(memory_space=pltpu.HBM)] * 2,
        out_specs=[pl.BlockSpec(memory_space=pltpu.VMEM)] * len(outs),
        out_shape=outs,
        scratch_shapes=[
            pltpu.VMEM((2,) + increment.shape, jnp.float32),
            pltpu.SemaphoreType.DMA((2, rows // CHUNK)),
        ],
        name="pack",
    )(increment, multiplier)


def sweep(src, dst, taps, first, last, blocks):
    center, c0, c1, c2, c3, c4, c5, c6, c7 = taps
    group = 4

    def rows_of(it, carry):
        i = first + it * group
        for b in range(blocks):
            j = 8 + 8 * b
            at = [src[i - 2 + r, j : j + 8, :] for r in range(group + 4)]
            for r in range(group):
                total = center * at[r + 2] + c0 * at[r]
                total = total + c1 * at[r + 1]
                total = total + c2 * at[r + 3]
                total = total + c3 * at[r + 4]
                total = total + c4 * src[i + r, j - 2 : j + 6, :]
                total = total + c5 * src[i + r, j - 1 : j + 7, :]
                total = total + c6 * src[i + r, j + 1 : j + 9, :]
                total = total + c7 * src[i + r, j + 2 : j + 10, :]
                dst[i + r, j : j + 8, :] = total
        return carry

    lax.fori_loop(0, (last - first) // group, rows_of, 0)


def transport_kernel(crossing, inc, mul, above, below, strip, above_corner, below_corner, rates, _, out, a, b):
    lat, lon = lax.axis_index("lat"), lax.axis_index("lon")
    odd = lax.rem(lax.axis_index("sub"), 2)
    n_lat = lax.axis_size("lat")
    rows, across = inc.shape[0], inc.shape[1]
    tall = rows + 2 * REACH
    blocks = (across + REACH) // 8
    own = pl.multiple_of(8 + REACH * lon, 8)
    beside = pl.multiple_of(8 + across * (1 - lon), 8)
    f = 1 - odd if crossing else odd
    forward = f == 0

    @pl.when(pl.program_id(0) == 0)
    def _():
        for buf in (a, b):
            for r in range(tall):
                buf[r] = jnp.zeros(buf.shape[1:], jnp.float32)

    for r in range(REACH):
        a[r, pl.ds(own, across), :] = above[f, r].astype(jnp.float32)
        a[rows + REACH + r, pl.ds(own, across), :] = below[f, r].astype(jnp.float32)
    for r in range(rows):
        a[REACH + r, pl.ds(beside, REACH), :] = strip[f, r].astype(jnp.float32)
    for r in range(EDGE):
        a[REACH - EDGE + r, pl.ds(beside, REACH), :] = above_corner[f, r].astype(jnp.float32)
        a[rows + REACH + r, pl.ds(beside, REACH), :] = below_corner[f, r].astype(jnp.float32)

    @pl.when(forward)
    def _():
        for r in range(rows):
            a[REACH + r, pl.ds(own, across), :] = inc[r]

    @pl.when(jnp.logical_not(forward))
    def _():
        for r in range(rows):
            a[REACH + r, pl.ds(own, across), :] = mul[r]

    spread = [
        jnp.broadcast_to(jnp.where(forward, rates[k : k + 1, :], rates[m : m + 1, :]), (8, LANES))
        for k, m in enumerate(MIRROR)
    ]
    rest = spread[0]
    for k in range(1, 8):
        rest = rest + spread[k]
    taps = [1.0 - rest] + spread

    for t in range(STEPS):
        first, last = 2 * (t + 1), tall - 2 * (t + 1)
        sweep(a, b, taps, first, last, blocks)
        if t < STEPS - 1:

            @pl.when(lat == 0)
            def _(b=b, first=first):
                for r in range(first, REACH):
                    b[r] = jnp.zeros(b.shape[1:], jnp.float32)

            @pl.when(lat == n_lat - 1)
            def _(b=b, last=last):
                for r in range(rows + REACH, last):
                    b[r] = jnp.zeros(b.shape[1:], jnp.float32)

        a, b = b, a

    for r in range(rows):
        out[r] = a[REACH + r, pl.ds(own, across), :].astype(jnp.bfloat16)


def transported(crossing, increment, multiplier, pieces, rates, token):
    rows, across, levels = increment.shape
    operands = (increment, multiplier, *pieces, rates)
    after = pl.BlockSpec(token.shape, lambda l: (0, 0))
    out = jax.ShapeDtypeStruct(increment.shape, jnp.bfloat16)
    return pl.pallas_call(
        functools.partial(transport_kernel, crossing),
        grid=(levels // LANES,),
        in_specs=[by_lanes(a) for a in operands] + [after],
        out_specs=by_lanes(out),
        out_shape=out,
        scratch_shapes=[pltpu.VMEM((rows + 2 * REACH, across + REACH + 16, LANES), jnp.float32)] * 2,
        compiler_params=pltpu.CompilerParams(vmem_limit_bytes=16 << 20),
        cost_estimate=pl.CostEstimate(flops=50_000_000, bytes_accessed=6 << 20, transcendentals=0),
        name="crossing" if crossing else "staying",
    )(*operands, token)


def final_kernel(inc, base, from_chip, from_core, error_out, grad_out):
    odd = lax.rem(lax.axis_index("sub"), 2) == 1
    group = 2
    for r in range(0, inc.shape[0], group):
        rows = slice(r, r + group)
        x = from_chip[rows].astype(jnp.float32)
        d = from_core[rows].astype(jnp.float32)
        error_out[rows] = inc[rows] - jnp.where(odd, d, x)
        grad_out[rows] = base[rows] - jnp.where(odd, x, d)


def final(increment, base, from_chip, from_core):
    rows, across, levels = increment.shape
    block = pl.BlockSpec((4, across, levels), lambda i: (i, 0, 0))
    return pl.pallas_call(
        final_kernel,
        grid=(rows // 4,),
        in_specs=[block] * 4,
        out_specs=[block] * 2,
        out_shape=[jax.ShapeDtypeStruct(increment.shape, jnp.float32)] * 2,
        compiler_params=pltpu.CompilerParams(vmem_limit_bytes=16 << 20),
        cost_estimate=pl.CostEstimate(flops=4_000_000, bytes_accessed=10 << 20, transcendentals=0),
        name="final",
    )(increment, base, from_chip, from_core)


ROWS_BY_COLS = (((1,), (1,)), ((), ()))


def network_kernel(
    count, columns, state, back, base, cot, hidden_weight, hidden_bias, output_weight,
    tangent_out, adjoint_out, token_out, tangents, column_of, slot_of,
):
    step = pl.program_id(0)
    slots = cot.shape[0]
    col_steps = tangents.shape[0] // COLS_TILE

    @pl.when(step == 0)
    def _():
        token_out[...] = jnp.zeros_like(token_out)
        alive = lax.broadcasted_iota(jnp.int32, (1, slots), 1) < count[0]
        named = jnp.where(alive, columns[...], -1)
        column_of[...] = jnp.broadcast_to(named, column_of.shape)
        for s in range(0, slots, LANES):
            piece = jnp.broadcast_to(named[:, s : s + LANES], (LANES, LANES))
            slot_of[s : s + LANES, :] = piece.T

    @pl.when(step < col_steps)
    def _():
        preact = jnp.dot(back[...], hidden_weight[...], preferred_element_type=jnp.float32) + hidden_bias[...]
        hidden = jnp.tanh(preact)
        slopes = 1.0 - hidden * hidden
        forward = jnp.dot(
            state[...].astype(jnp.bfloat16), hidden_weight[...], preferred_element_type=jnp.float32
        )
        scaled = (slopes * forward).astype(jnp.bfloat16)
        tangent = jnp.dot(scaled, output_weight[...], preferred_element_type=jnp.float32)
        start = pl.multiple_of(step * COLS_TILE, COLS_TILE)
        tangents[pl.ds(start, COLS_TILE), :] = tangent.astype(jnp.bfloat16)
        ids = lax.broadcasted_iota(jnp.int32, (COLS_TILE, slots), 0) + start
        picks = jnp.where(column_of[0:1, :] == ids, 1.0, 0.0).astype(jnp.bfloat16)
        gathered = jnp.dot(picks, cot[...], preferred_element_type=jnp.float32).astype(jnp.bfloat16)
        pulled = lax.dot_general(gathered, output_weight[...], ROWS_BY_COLS, preferred_element_type=jnp.float32)
        weighted = (slopes * pulled).astype(jnp.bfloat16)
        adjoint_out[...] = base[...] + lax.dot_general(
            weighted, hidden_weight[...], ROWS_BY_COLS, preferred_element_type=jnp.float32
        )

    @pl.when(step >= col_steps)
    def _():
        start = pl.multiple_of((step - col_steps) * SLOTS_TILE, SLOTS_TILE)
        mine = slot_of[pl.ds(start, SLOTS_TILE), :]
        lane = lax.broadcasted_iota(jnp.int32, mine.shape, 1)
        picks = jnp.concatenate(
            [
                jnp.where(mine == lane + k, 1.0, 0.0).astype(jnp.bfloat16)
                for k in range(0, tangents.shape[0], LANES)
            ],
            axis=1,
        )
        tangent_out[...] = jnp.dot(picks, tangents[...], preferred_element_type=jnp.float32).astype(jnp.bfloat16)


def network(count, columns, state, back, base, cot, hidden_weight, hidden_bias, output_weight):
    cols, levels = state.shape
    slots, chan = cot.shape
    col_steps, slot_steps = cols // COLS_TILE, slots // SLOTS_TILE
    whole = lambda a: pl.BlockSpec(a.shape, lambda i: (0, 0))
    by_cols = lambda width: pl.BlockSpec((COLS_TILE, width), lambda i: (jnp.minimum(i, col_steps - 1), 0))
    units = 5 * cols + 2 * slots
    return pl.pallas_call(
        network_kernel,
        grid=(col_steps + slot_steps,),
        in_specs=[
            pl.BlockSpec(memory_space=pltpu.SMEM),
            whole(columns),
            by_cols(levels),
            by_cols(levels),
            by_cols(levels),
            whole(cot),
            whole(hidden_weight),
            whole(hidden_bias),
            whole(output_weight),
        ],
        out_specs=[
            pl.BlockSpec((SLOTS_TILE, chan), lambda i: (jnp.maximum(i - col_steps, 0), 0)),
            by_cols(levels),
            pl.BlockSpec((8, LANES), lambda i: (0, 0)),
        ],
        out_shape=[
            jax.ShapeDtypeStruct((slots, chan), jnp.bfloat16),
            jax.ShapeDtypeStruct((cols, levels), jnp.float32),
            jax.ShapeDtypeStruct((8, LANES), jnp.float32),
        ],
        scratch_shapes=[
            pltpu.VMEM((cols, chan), jnp.bfloat16),
            pltpu.VMEM((8, slots), jnp.int32),
            pltpu.VMEM((slots, LANES), jnp.int32),
        ],
        cost_estimate=pl.CostEstimate(
            flops=2 * units * levels * hidden_bias.shape[1], bytes_accessed=12 << 20, transcendentals=1 << 20
        ),
        name="network",
    )(count, columns, state, back, base, cot, hidden_weight, hidden_bias, output_weight)


def sent(array, to):
    counts = [lax.axis_size(axis) for axis in ("sub", "lat", "lon")]
    flat = lambda s, a, o: (s * counts[1] + a) * counts[2] + o
    pairs = []
    for s in range(counts[0]):
        for a in range(counts[1]):
            for o in range(counts[2]):
                target = to(s, a, o)
                if all(0 <= t < n for t, n in zip(target, counts)):
                    pairs.append((flat(s, a, o), flat(*target)))
    return lax.ppermute(array, ("sub", "lat", "lon"), pairs)


def local(
    increment,
    multiplier,
    background,
    obs_cotangent,
    obs_column,
    obs_count,
    transport,
    hidden_weight,
    hidden_bias,
    output_weight,
):
    increment, multiplier = increment[0], multiplier[0]
    levels = increment.shape[2]
    low, high, strip, low_corner, high_corner = pack(increment, multiplier)
    above = sent(high, lambda s, a, o: (s, a + 1, o))
    below = sent(low, lambda s, a, o: (s, a - 1, o))
    pieces = [
        above,
        below,
        sent(strip, lambda s, a, o: (s, a, 1 - o)),
        sent(high_corner, lambda s, a, o: (s, a + 1, 1 - o)),
        sent(low_corner, lambda s, a, o: (s, a - 1, 1 - o)),
    ]
    myself = lax.axis_index(("lat", "lon"))
    my_count = lax.dynamic_slice(obs_count[0], (myself,), (1,))
    tangent, base, token = network(
        my_count,
        obs_column[0],
        increment.reshape(-1, levels),
        background[0].reshape(-1, levels),
        multiplier.reshape(-1, levels),
        obs_cotangent[0, 0],
        hidden_weight,
        hidden_bias[None, :],
        output_weight,
    )
    crossing = transported(True, increment, multiplier, pieces, transport, token)
    from_chip = sent(crossing, lambda s, a, o: (s + 1 if s % 2 else s - 1, a, o))
    staying = transported(False, increment, multiplier, pieces, transport, token)
    from_core = sent(staying, lambda s, a, o: (s - 1 if s % 2 else s + 1, a, o))
    model_error, gradient = final(increment, base.reshape(increment.shape), from_chip, from_core)
    return (model_error[None], gradient[None], tangent[None, None])


def solution(mesh):
    in_specs = (
        P("sub", "lat", "lon", None),
        P("sub", "lat", "lon", None),
        P("sub", "lat", "lon", None),
        P("sub", ("lat", "lon"), None, None),
        P("sub", ("lat", "lon"), None),
        P("sub", None),
        P(),
        P(),
        P(),
        P(),
    )
    out_specs = (
        P("sub", "lat", "lon", None),
        P("sub", "lat", "lon", None),
        P("sub", ("lat", "lon"), None, None),
    )
    return jax.shard_map(local, mesh=mesh, in_specs=in_specs, out_specs=out_specs, check_vma=False)
```

```python
import functools

import jax
import jax.numpy as jnp
from jax import lax
from jax.experimental import pallas as pl
from jax.experimental.pallas import tpu as pltpu
from jax.sharding import PartitionSpec as P


STEPS = 4
REACH = 2 * STEPS
EDGE = REACH - 2
LANES = 128
COLS_TILE = 256
SLOTS_TILE = 512
MIRROR = (3, 2, 1, 0, 7, 6, 5, 4)
TOKEN = jax.ShapeDtypeStruct((8, LANES), jnp.float32)


CHUNK = 4


def pack_kernel(inc, mul, low, high, strip, held, sems):
    lon = lax.axis_index("lon")
    rows, across = inc.shape[0], inc.shape[1]
    side = pl.multiple_of((across - REACH) * (1 - lon), REACH)
    copies = {}
    for start in range(0, rows, CHUNK):
        for f, src in enumerate((inc, mul)):
            part = pl.ds(start, CHUNK)
            copies[f, start] = pltpu.make_async_copy(src.at[part], held.at[f, part], sems.at[f, start // CHUNK])
            copies[f, start].start()
    for start in range(0, rows, CHUNK):
        for f in range(2):
            copies[f, start].wait()
            for r in range(start, start + CHUNK):
                row = held[f, r].astype(jnp.bfloat16)
                if r < REACH:
                    low[f, r] = row
                if r >= rows - REACH:
                    high[f, r - rows + REACH] = row
                strip[f, r] = held[f, r, pl.ds(side, REACH), :].astype(jnp.bfloat16)


def pack(increment, multiplier):
    rows, across, levels = increment.shape
    shapes = [(2, REACH, across), (2, REACH, across), (2, rows, REACH)]
    return pl.pallas_call(
        pack_kernel,
        in_specs=[pl.BlockSpec(memory_space=pltpu.HBM)] * 2,
        out_specs=[pl.BlockSpec(memory_space=pltpu.VMEM)] * 3,
        out_shape=[jax.ShapeDtypeStruct(s + (levels,), jnp.bfloat16) for s in shapes],
        scratch_shapes=[
            pltpu.VMEM((2,) + increment.shape, jnp.float32),
            pltpu.SemaphoreType.DMA((2, rows // CHUNK)),
        ],
        name="pack",
    )(increment, multiplier)


def corner_kernel(strip, _, low, high, token):
    rows = strip.shape[1]
    low[...] = strip[:, :EDGE]
    high[...] = strip[:, rows - EDGE :]
    token[...] = jnp.zeros_like(token)


def corners(strip, token):
    fields, _, wide, levels = strip.shape
    return pl.pallas_call(
        corner_kernel,
        out_shape=[jax.ShapeDtypeStruct((fields, EDGE, wide, levels), jnp.bfloat16)] * 2 + [TOKEN],
        compiler_params=pltpu.CompilerParams(vmem_limit_bytes=8 << 20),
        name="corners",
    )(strip, token)


def sweep(src, dst, taps, first, last, blocks):
    c0, c1, c2, c3, c4, c5, c6, c7 = taps
    group = 4

    def rows_of(it, carry):
        i = first + it * group
        for b in range(blocks):
            j = 8 + 8 * b
            at = [src[i - 2 + r, j : j + 8, :] for r in range(group + 4)]
            for r in range(group):
                total = at[r + 2] + c0 * at[r]
                total = total + c1 * at[r + 1]
                total = total + c2 * at[r + 3]
                total = total + c3 * at[r + 4]
                total = total + c4 * src[i + r, j - 2 : j + 6, :]
                total = total + c5 * src[i + r, j - 1 : j + 7, :]
                total = total + c6 * src[i + r, j + 1 : j + 9, :]
                total = total + c7 * src[i + r, j + 2 : j + 10, :]
                dst[i + r, j : j + 8, :] = total
        return carry

    lax.fori_loop(0, (last - first) // group, rows_of, 0)


def transport_kernel(
    crossing, inc, mul, above, below, strip, above_corner, below_corner, rates, _, out, token, bufs, other, sems
):
    lat, lon = lax.axis_index("lat"), lax.axis_index("lon")
    odd = lax.rem(lax.axis_index("sub"), 2)
    n_lat = lax.axis_size("lat")
    rows, across, levels = inc.shape
    tall = rows + 2 * REACH
    blocks = (across + REACH) // 8
    tiles = levels // LANES
    own = pl.multiple_of(8 + REACH * lon, 8)
    beside = pl.multiple_of(8 + across * (1 - lon), 8)
    f = 1 - odd if crossing else odd
    forward = f == 0

    def arriving(src, t):
        there = bufs.at[t, pl.ds(REACH, rows), pl.ds(own, across), :]
        return pltpu.make_async_copy(src.at[:, :, pl.ds(t * LANES, LANES)], there, sems.at[t])

    @pl.when(forward)
    def _():
        for t in range(tiles):
            arriving(inc, t).start()

    @pl.when(jnp.logical_not(forward))
    def _():
        for t in range(tiles):
            arriving(mul, t).start()

    token[...] = jnp.zeros_like(token)
    blank = jnp.zeros((8, LANES), jnp.float32)
    for r in range(tall):
        other[r] = jnp.zeros(other.shape[1:], jnp.float32)
        for t in range(tiles):
            bufs[t, r, 0:8, :] = blank
            bufs[t, r, 8 * blocks + 8 : 8 * blocks + 16, :] = blank
    for t in range(tiles):
        for r in (0, 1, tall - 2, tall - 1):
            bufs[t, r, pl.ds(beside, REACH), :] = blank
        for r in range(REACH):
            lanes = slice(t * LANES, (t + 1) * LANES)
            bufs[t, r, pl.ds(own, across), :] = above[f, r, :, lanes].astype(jnp.float32)
            bufs[t, rows + REACH + r, pl.ds(own, across), :] = below[f, r, :, lanes].astype(jnp.float32)
        for r in range(rows):
            bufs[t, REACH + r, pl.ds(beside, REACH), :] = strip[f, r, :, lanes].astype(jnp.float32)
        for r in range(EDGE):
            bufs[t, REACH - EDGE + r, pl.ds(beside, REACH), :] = above_corner[f, r, :, lanes].astype(jnp.float32)
            bufs[t, rows + REACH + r, pl.ds(beside, REACH), :] = below_corner[f, r, :, lanes].astype(jnp.float32)

    def tile_of(t, carry):
        lanes = pl.ds(pl.multiple_of(t * LANES, LANES), LANES)
        pltpu.make_async_copy(
            inc.at[:, :, lanes], bufs.at[t, pl.ds(REACH, rows), pl.ds(own, across), :], sems.at[t]
        ).wait()
        spread = [
            jnp.broadcast_to(jnp.where(forward, rates[k : k + 1, lanes], rates[m : m + 1, lanes]), (8, LANES))
            for k, m in enumerate(MIRROR)
        ]
        rest = spread[0]
        for k in range(1, 8):
            rest = rest + spread[k]
        center = 1.0 - rest
        taps = [c / center for c in spread]
        scale = (center * center) * (center * center)
        a, b = bufs.at[t], other
        for step in range(STEPS):
            first, last = 2 * (step + 1), tall - 2 * (step + 1)
            sweep(a, b, taps, first, last, blocks)
            if step < STEPS - 1:

                @pl.when(lat == 0)
                def _(b=b, first=first):
                    for r in range(first, REACH):
                        b[r] = jnp.zeros(b.shape[1:], jnp.float32)

                @pl.when(lat == n_lat - 1)
                def _(b=b, last=last):
                    for r in range(rows + REACH, last):
                        b[r] = jnp.zeros(b.shape[1:], jnp.float32)

            a, b = b, a
        for r in range(rows):
            out[r, :, lanes] = (scale[0:1] * a[REACH + r, pl.ds(own, across), :]).astype(jnp.bfloat16)
        return carry

    lax.fori_loop(0, tiles, tile_of, 0)


def transported(crossing, increment, multiplier, pieces, rates, token):
    rows, across, levels = increment.shape
    tall, wide, tiles = rows + 2 * REACH, across + REACH + 16, levels // LANES
    hbm, vmem = pl.BlockSpec(memory_space=pltpu.HBM), pl.BlockSpec(memory_space=pltpu.VMEM)
    return pl.pallas_call(
        functools.partial(transport_kernel, crossing),
        in_specs=[hbm, hbm] + [vmem] * (len(pieces) + 2),
        out_specs=[vmem, vmem],
        out_shape=[jax.ShapeDtypeStruct(increment.shape, jnp.bfloat16), TOKEN],
        scratch_shapes=[
            pltpu.VMEM((tiles, tall, wide, LANES), jnp.float32),
            pltpu.VMEM((tall, wide, LANES), jnp.float32),
            pltpu.SemaphoreType.DMA((tiles,)),
        ],
        compiler_params=pltpu.CompilerParams(vmem_limit_bytes=24 << 20),
        cost_estimate=pl.CostEstimate(flops=50_000_000, bytes_accessed=6 << 20, transcendentals=0),
        name="crossing" if crossing else "staying",
    )(increment, multiplier, *pieces, rates, token)


def final_kernel(inc, base, from_chip, from_core, error_out, grad_out):
    odd = lax.rem(lax.axis_index("sub"), 2) == 1
    group = 2
    for r in range(0, inc.shape[0], group):
        rows = slice(r, r + group)
        x = from_chip[rows].astype(jnp.float32)
        d = from_core[rows].astype(jnp.float32)
        error_out[rows] = inc[rows] - jnp.where(odd, d, x)
        grad_out[rows] = base[rows] - jnp.where(odd, x, d)


def final(increment, base, from_chip, from_core):
    rows, across, levels = increment.shape
    block = pl.BlockSpec((4, across, levels), lambda i: (i, 0, 0))
    return pl.pallas_call(
        final_kernel,
        grid=(rows // 4,),
        in_specs=[block] * 4,
        out_specs=[block] * 2,
        out_shape=[jax.ShapeDtypeStruct(increment.shape, jnp.float32)] * 2,
        compiler_params=pltpu.CompilerParams(vmem_limit_bytes=16 << 20),
        cost_estimate=pl.CostEstimate(flops=4_000_000, bytes_accessed=10 << 20, transcendentals=0),
        name="final",
    )(increment, base, from_chip, from_core)


ROWS_BY_COLS = (((1,), (1,)), ((), ()))


def network_kernel(
    count, columns, hidden_bias, state_in, back_in, base_in, cot_in, hidden_in, output_in,
    tangents, base_out, token,
    state, back, base, cot, hidden_weight, output_weight, sems, out_sems,
):
    cols, slots = state.shape[0], cot.shape[0]
    moves = [
        (hidden_in, hidden_weight), (back_in, back), (state_in, state),
        (output_in, output_weight), (cot_in, cot), (base_in, base),
    ]
    copies = [pltpu.make_async_copy(a, b, sems.at[i]) for i, (a, b) in enumerate(moves)]
    for copy in copies:
        copy.start()
    token[...] = jnp.zeros_like(token)
    alive = lax.broadcasted_iota(jnp.int32, (1, slots), 1) < count[0]
    named = jnp.where(alive, columns[...], -1)
    outs = []
    for i, start in enumerate(range(0, cols, COLS_TILE)):
        rows = slice(start, start + COLS_TILE)
        if i == 0:
            copies[0].wait()
            copies[1].wait()
        preact = jnp.dot(back[rows], hidden_weight[...], preferred_element_type=jnp.float32) + hidden_bias[...]
        hidden = jnp.tanh(preact)
        slopes = 1.0 - hidden * hidden
        if i == 0:
            copies[2].wait()
        forward = jnp.dot(state[rows].astype(jnp.bfloat16), hidden_weight[...], preferred_element_type=jnp.float32)
        scaled = (slopes * forward).astype(jnp.bfloat16)
        if i == 0:
            copies[3].wait()
        tangent = jnp.dot(scaled, output_weight[...], preferred_element_type=jnp.float32)
        tangents[rows] = tangent.astype(jnp.bfloat16)
        ids = lax.broadcasted_iota(jnp.int32, (COLS_TILE, slots), 0) + start
        picks = jnp.where(named == ids, 1.0, 0.0).astype(jnp.bfloat16)
        if i == 0:
            copies[4].wait()
        gathered = jnp.dot(picks, cot[...], preferred_element_type=jnp.float32).astype(jnp.bfloat16)
        pulled = lax.dot_general(gathered, output_weight[...], ROWS_BY_COLS, preferred_element_type=jnp.float32)
        weighted = (slopes * pulled).astype(jnp.bfloat16)
        adjoint = lax.dot_general(weighted, hidden_weight[...], ROWS_BY_COLS, preferred_element_type=jnp.float32)
        if i == 0:
            copies[5].wait()
        base[rows] = base[rows] + adjoint
        outs.append(pltpu.make_async_copy(base.at[rows], base_out.at[rows], out_sems.at[i]))
        outs[-1].start()
    for out in outs:
        out.wait()


def network(count, columns, state, back, base, cot, hidden_weight, hidden_bias, output_weight):
    cols, levels = state.shape
    slots, chan = cot.shape
    hbm, vmem = pl.BlockSpec(memory_space=pltpu.HBM), pl.BlockSpec(memory_space=pltpu.VMEM)
    moved = (state, back, base, cot, hidden_weight, output_weight)
    return pl.pallas_call(
        network_kernel,
        in_specs=[pl.BlockSpec(memory_space=pltpu.SMEM), vmem, vmem] + [hbm] * 6,
        out_specs=[vmem, hbm, vmem],
        out_shape=[
            jax.ShapeDtypeStruct((cols, chan), jnp.bfloat16),
            jax.ShapeDtypeStruct((cols, levels), jnp.float32),
            TOKEN,
        ],
        scratch_shapes=[pltpu.VMEM(a.shape, a.dtype) for a in moved]
        + [pltpu.SemaphoreType.DMA((6,)), pltpu.SemaphoreType.DMA((cols // COLS_TILE,))],
        cost_estimate=pl.CostEstimate(
            flops=2 * (5 * cols + slots) * levels * hidden_bias.shape[1],
            bytes_accessed=12 << 20,
            transcendentals=1 << 20,
        ),
        name="network",
    )(count, columns, hidden_bias, *moved)


def spread_kernel(count, columns, tangents, _, out, token, held, sems):
    slots, cols = held.shape[0], tangents.shape[0]
    token[...] = jnp.zeros_like(token)
    lane = lax.broadcasted_iota(jnp.int32, (LANES, LANES), 1)
    outs = []
    for i, start in enumerate(range(0, slots, SLOTS_TILE)):
        rows = slice(start, start + SLOTS_TILE)
        parts = []
        for s in range(start, start + SLOTS_TILE, LANES):
            alive = lax.broadcasted_iota(jnp.int32, (1, LANES), 1) + s < count[0]
            named = jnp.where(alive, columns[:, s : s + LANES], -1)
            mine = jnp.broadcast_to(named, (LANES, LANES)).T
            hits = [jnp.where(mine == lane + k, 1.0, 0.0).astype(jnp.bfloat16) for k in range(0, cols, LANES)]
            parts.append(jnp.concatenate(hits, axis=1))
        picks = jnp.concatenate(parts, axis=0)
        held[rows] = jnp.dot(picks, tangents[...], preferred_element_type=jnp.float32).astype(jnp.bfloat16)
        outs.append(pltpu.make_async_copy(held.at[rows], out.at[rows], sems.at[i]))
        outs[-1].start()
    for copy in outs:
        copy.wait()


def spread(count, columns, tangents, token):
    slots, (cols, chan) = columns.shape[1], tangents.shape
    vmem = pl.BlockSpec(memory_space=pltpu.VMEM)
    return pl.pallas_call(
        spread_kernel,
        in_specs=[pl.BlockSpec(memory_space=pltpu.SMEM), vmem, vmem, vmem],
        out_specs=[pl.BlockSpec(memory_space=pltpu.HBM), vmem],
        out_shape=[jax.ShapeDtypeStruct((slots, chan), jnp.bfloat16), TOKEN],
        scratch_shapes=[
            pltpu.VMEM((slots, chan), jnp.bfloat16),
            pltpu.SemaphoreType.DMA((slots // SLOTS_TILE,)),
        ],
        compiler_params=pltpu.CompilerParams(vmem_limit_bytes=24 << 20),
        cost_estimate=pl.CostEstimate(flops=2 * slots * cols * chan, bytes_accessed=4 << 20, transcendentals=0),
        name="spread",
    )(count, columns, tangents, token)


def sent(array, to):
    counts = [lax.axis_size(axis) for axis in ("sub", "lat", "lon")]
    flat = lambda s, a, o: (s * counts[1] + a) * counts[2] + o
    pairs = []
    for s in range(counts[0]):
        for a in range(counts[1]):
            for o in range(counts[2]):
                target = to(s, a, o)
                if all(0 <= t < n for t, n in zip(target, counts)):
                    pairs.append((flat(s, a, o), flat(*target)))
    return lax.ppermute(array, ("sub", "lat", "lon"), pairs)


def local(
    increment,
    multiplier,
    background,
    obs_cotangent,
    obs_column,
    obs_count,
    transport,
    hidden_weight,
    hidden_bias,
    output_weight,
):
    increment, multiplier = increment[0], multiplier[0]
    levels = increment.shape[2]
    low, high, strip = pack(increment, multiplier)
    across = sent(strip, lambda s, a, o: (s, a, 1 - o))
    above = sent(high, lambda s, a, o: (s, a + 1, o))
    below = sent(low, lambda s, a, o: (s, a - 1, o))
    myself = lax.axis_index(("lat", "lon"))
    my_count = lax.dynamic_slice(obs_count[0], (myself,), (1,))
    tangents, base, token = network(
        my_count,
        obs_column[0],
        increment.reshape(-1, levels),
        background[0].reshape(-1, levels),
        multiplier.reshape(-1, levels),
        obs_cotangent[0, 0],
        hidden_weight,
        hidden_bias[None, :],
        output_weight,
    )
    low_corner, high_corner, token = corners(across, token)
    above_corner = sent(high_corner, lambda s, a, o: (s, a + 1, o))
    below_corner = sent(low_corner, lambda s, a, o: (s, a - 1, o))
    tangent, token = spread(my_count, obs_column[0], tangents, token)
    pieces = [above, below, across, above_corner, below_corner]
    crossing, token = transported(True, increment, multiplier, pieces, transport, token)
    from_chip = sent(crossing, lambda s, a, o: (s + 1 if s % 2 else s - 1, a, o))
    staying, _ = transported(False, increment, multiplier, pieces, transport, token)
    from_core = sent(staying, lambda s, a, o: (s - 1 if s % 2 else s + 1, a, o))
    model_error, gradient = final(increment, base.reshape(increment.shape), from_chip, from_core)
    return (model_error[None], gradient[None], tangent[None, None])


def solution(mesh):
    in_specs = (
        P("sub", "lat", "lon", None),
        P("sub", "lat", "lon", None),
        P("sub", "lat", "lon", None),
        P("sub", ("lat", "lon"), None, None),
        P("sub", ("lat", "lon"), None),
        P("sub", None),
        P(),
        P(),
        P(),
        P(),
    )
    out_specs = (
        P("sub", "lat", "lon", None),
        P("sub", "lat", "lon", None),
        P("sub", ("lat", "lon"), None, None),
    )
    return jax.shard_map(local, mesh=mesh, in_specs=in_specs, out_specs=out_specs, check_vma=False)
```

```python
import functools

import jax
import jax.numpy as jnp
from jax import lax
from jax.experimental import pallas as pl
from jax.experimental.pallas import tpu as pltpu
from jax.sharding import PartitionSpec as P


STEPS = 4
REACH = 2 * STEPS
EDGE = REACH - 2
LANES = 128
COLS_TILE = 256
SLOTS_TILE = 512
MIRROR = (3, 2, 1, 0, 7, 6, 5, 4)
TOKEN = jax.ShapeDtypeStruct((8, LANES), jnp.float32)


CHUNK = 4


def in_hbm(*arrays):
    return [pltpu.with_memory_space_constraint(a, pltpu.HBM) for a in arrays]


def pack_kernel(inc, mul, low, high, strip, held, sems):
    lon = lax.axis_index("lon")
    rows, across = inc.shape[0], inc.shape[1]
    side = pl.multiple_of((across - REACH) * (1 - lon), REACH)
    copies = {}
    for start in range(0, rows, CHUNK):
        for f, src in enumerate((inc, mul)):
            part = pl.ds(start, CHUNK)
            copies[f, start] = pltpu.make_async_copy(src.at[part], held.at[f, part], sems.at[f, start // CHUNK])
            copies[f, start].start()
    for start in range(0, rows, CHUNK):
        for f in range(2):
            copies[f, start].wait()
            for r in range(start, start + CHUNK):
                row = held[f, r].astype(jnp.bfloat16)
                if r < REACH:
                    low[f, r] = row
                if r >= rows - REACH:
                    high[f, r - rows + REACH] = row
                strip[f, r] = held[f, r, pl.ds(side, REACH), :].astype(jnp.bfloat16)


def pack(increment, multiplier):
    rows, across, levels = increment.shape
    shapes = [(2, REACH, across), (2, REACH, across), (2, rows, REACH)]
    return pl.pallas_call(
        pack_kernel,
        in_specs=[pl.BlockSpec(memory_space=pltpu.HBM)] * 2,
        out_specs=[pl.BlockSpec(memory_space=pltpu.VMEM)] * 3,
        out_shape=[jax.ShapeDtypeStruct(s + (levels,), jnp.bfloat16) for s in shapes],
        scratch_shapes=[
            pltpu.VMEM((2,) + increment.shape, jnp.float32),
            pltpu.SemaphoreType.DMA((2, rows // CHUNK)),
        ],
        compiler_params=pltpu.CompilerParams(vmem_limit_bytes=16 << 20),
        name="pack",
    )(*in_hbm(increment, multiplier))


def corner_kernel(strip, _, low, high, token):
    rows = strip.shape[1]
    low[...] = strip[:, :EDGE]
    high[...] = strip[:, rows - EDGE :]
    token[...] = jnp.zeros_like(token)


def corners(strip, token):
    fields, _, wide, levels = strip.shape
    return pl.pallas_call(
        corner_kernel,
        in_specs=[pl.BlockSpec(memory_space=pltpu.VMEM), pl.BlockSpec(memory_space=pl.ANY)],
        out_shape=[jax.ShapeDtypeStruct((fields, EDGE, wide, levels), jnp.bfloat16)] * 2 + [TOKEN],
        compiler_params=pltpu.CompilerParams(vmem_limit_bytes=8 << 20),
        name="corners",
    )(strip, token)


def sweep(src, dst, taps, first, last, blocks):
    c0, c1, c2, c3, c4, c5, c6, c7 = taps
    group = 4

    def rows_of(it, carry):
        i = first + it * group
        for b in range(blocks):
            j = 8 + 8 * b
            at = [src[i - 2 + r, j : j + 8, :] for r in range(group + 4)]
            for r in range(group):
                total = at[r + 2] + c0 * at[r]
                total = total + c1 * at[r + 1]
                total = total + c2 * at[r + 3]
                total = total + c3 * at[r + 4]
                total = total + c4 * src[i + r, j - 2 : j + 6, :]
                total = total + c5 * src[i + r, j - 1 : j + 7, :]
                total = total + c6 * src[i + r, j + 1 : j + 9, :]
                total = total + c7 * src[i + r, j + 2 : j + 10, :]
                dst[i + r, j : j + 8, :] = total
        return carry

    lax.fori_loop(0, (last - first) // group, rows_of, 0)


def transport_kernel(
    crossing, inc, mul, above, below, strip, above_corner, below_corner, rates, _, out, token, bufs, other, sems
):
    lat, lon = lax.axis_index("lat"), lax.axis_index("lon")
    odd = lax.rem(lax.axis_index("sub"), 2)
    n_lat = lax.axis_size("lat")
    rows, across, levels = inc.shape
    tall = rows + 2 * REACH
    blocks = (across + REACH) // 8
    tiles = levels // LANES
    own = pl.multiple_of(8 + REACH * lon, 8)
    beside = pl.multiple_of(8 + across * (1 - lon), 8)
    f = 1 - odd if crossing else odd
    forward = f == 0

    def arriving(src, t):
        there = bufs.at[t, pl.ds(REACH, rows), pl.ds(own, across), :]
        return pltpu.make_async_copy(src.at[:, :, pl.ds(t * LANES, LANES)], there, sems.at[t])

    @pl.when(forward)
    def _():
        for t in range(tiles):
            arriving(inc, t).start()

    @pl.when(jnp.logical_not(forward))
    def _():
        for t in range(tiles):
            arriving(mul, t).start()

    token[...] = jnp.zeros_like(token)
    blank = jnp.zeros((8, LANES), jnp.float32)
    for r in range(tall):
        other[r] = jnp.zeros(other.shape[1:], jnp.float32)
        for t in range(tiles):
            bufs[t, r, 0:8, :] = blank
            bufs[t, r, 8 * blocks + 8 : 8 * blocks + 16, :] = blank
    for t in range(tiles):
        for r in (0, 1, tall - 2, tall - 1):
            bufs[t, r, pl.ds(beside, REACH), :] = blank
        for r in range(REACH):
            lanes = slice(t * LANES, (t + 1) * LANES)
            bufs[t, r, pl.ds(own, across), :] = above[f, r, :, lanes].astype(jnp.float32)
            bufs[t, rows + REACH + r, pl.ds(own, across), :] = below[f, r, :, lanes].astype(jnp.float32)
        for r in range(rows):
            bufs[t, REACH + r, pl.ds(beside, REACH), :] = strip[f, r, :, lanes].astype(jnp.float32)
        for r in range(EDGE):
            bufs[t, REACH - EDGE + r, pl.ds(beside, REACH), :] = above_corner[f, r, :, lanes].astype(jnp.float32)
            bufs[t, rows + REACH + r, pl.ds(beside, REACH), :] = below_corner[f, r, :, lanes].astype(jnp.float32)

    def tile_of(t, carry):
        lanes = pl.ds(pl.multiple_of(t * LANES, LANES), LANES)
        pltpu.make_async_copy(
            inc.at[:, :, lanes], bufs.at[t, pl.ds(REACH, rows), pl.ds(own, across), :], sems.at[t]
        ).wait()
        spread = [
            jnp.broadcast_to(jnp.where(forward, rates[k : k + 1, lanes], rates[m : m + 1, lanes]), (8, LANES))
            for k, m in enumerate(MIRROR)
        ]
        rest = spread[0]
        for k in range(1, 8):
            rest = rest + spread[k]
        center = 1.0 - rest
        taps = [c / center for c in spread]
        scale = (center * center) * (center * center)
        a, b = bufs.at[t], other
        for step in range(STEPS):
            first, last = 2 * (step + 1), tall - 2 * (step + 1)
            sweep(a, b, taps, first, last, blocks)
            if step < STEPS - 1:

                @pl.when(lat == 0)
                def _(b=b, first=first):
                    for r in range(first, REACH):
                        b[r] = jnp.zeros(b.shape[1:], jnp.float32)

                @pl.when(lat == n_lat - 1)
                def _(b=b, last=last):
                    for r in range(rows + REACH, last):
                        b[r] = jnp.zeros(b.shape[1:], jnp.float32)

            a, b = b, a
        for r in range(rows):
            out[r, :, lanes] = (scale[0:1] * a[REACH + r, pl.ds(own, across), :]).astype(jnp.bfloat16)
        return carry

    lax.fori_loop(0, tiles, tile_of, 0)


def transported(crossing, increment, multiplier, pieces, rates, token):
    rows, across, levels = increment.shape
    tall, wide, tiles = rows + 2 * REACH, across + REACH + 16, levels // LANES
    hbm, vmem = pl.BlockSpec(memory_space=pltpu.HBM), pl.BlockSpec(memory_space=pltpu.VMEM)
    return pl.pallas_call(
        functools.partial(transport_kernel, crossing),
        in_specs=[hbm, hbm] + [vmem] * (len(pieces) + 1) + [pl.BlockSpec(memory_space=pl.ANY)],
        out_specs=[vmem, vmem],
        out_shape=[jax.ShapeDtypeStruct(increment.shape, jnp.bfloat16), TOKEN],
        scratch_shapes=[
            pltpu.VMEM((tiles, tall, wide, LANES), jnp.float32),
            pltpu.VMEM((tall, wide, LANES), jnp.float32),
            pltpu.SemaphoreType.DMA((tiles,)),
        ],
        compiler_params=pltpu.CompilerParams(vmem_limit_bytes=24 << 20),
        cost_estimate=pl.CostEstimate(flops=50_000_000, bytes_accessed=6 << 20, transcendentals=0),
        name="crossing" if crossing else "staying",
    )(*in_hbm(increment, multiplier), *pieces, rates, token)


def final_kernel(inc, base, from_chip, from_core, error_out, grad_out):
    odd = lax.rem(lax.axis_index("sub"), 2) == 1
    group = 2
    for r in range(0, inc.shape[0], group):
        rows = slice(r, r + group)
        x = from_chip[rows].astype(jnp.float32)
        d = from_core[rows].astype(jnp.float32)
        error_out[rows] = inc[rows] - jnp.where(odd, d, x)
        grad_out[rows] = base[rows] - jnp.where(odd, x, d)


def final(increment, base, from_chip, from_core):
    rows, across, levels = increment.shape
    block = pl.BlockSpec((4, across, levels), lambda i: (i, 0, 0))
    return pl.pallas_call(
        final_kernel,
        grid=(rows // 4,),
        in_specs=[block] * 4,
        out_specs=[block] * 2,
        out_shape=[jax.ShapeDtypeStruct(increment.shape, jnp.float32)] * 2,
        compiler_params=pltpu.CompilerParams(vmem_limit_bytes=16 << 20),
        cost_estimate=pl.CostEstimate(flops=4_000_000, bytes_accessed=10 << 20, transcendentals=0),
        name="final",
    )(increment, base, from_chip, from_core)


ROWS_BY_COLS = (((1,), (1,)), ((), ()))


def network_kernel(
    count, columns, hidden_bias, state_in, back_in, base_in, cot_in, hidden_in, output_in,
    tangents, base_out, token,
    state, back, base, cot, hidden_weight, output_weight, sems, out_sems,
):
    cols, slots = state.shape[0], cot.shape[0]
    moves = [
        (hidden_in, hidden_weight), (back_in, back), (state_in, state),
        (output_in, output_weight), (cot_in, cot), (base_in, base),
    ]
    copies = [pltpu.make_async_copy(a, b, sems.at[i]) for i, (a, b) in enumerate(moves)]
    for copy in copies:
        copy.start()
    token[...] = jnp.zeros_like(token)
    alive = lax.broadcasted_iota(jnp.int32, (1, slots), 1) < count[0]
    named = jnp.where(alive, columns[...], -1)
    outs = []
    for i, start in enumerate(range(0, cols, COLS_TILE)):
        rows = slice(start, start + COLS_TILE)
        if i == 0:
            copies[0].wait()
            copies[1].wait()
        preact = jnp.dot(back[rows], hidden_weight[...], preferred_element_type=jnp.float32) + hidden_bias[...]
        hidden = jnp.tanh(preact)
        slopes = 1.0 - hidden * hidden
        if i == 0:
            copies[2].wait()
        forward = jnp.dot(state[rows].astype(jnp.bfloat16), hidden_weight[...], preferred_element_type=jnp.float32)
        scaled = (slopes * forward).astype(jnp.bfloat16)
        if i == 0:
            copies[3].wait()
        tangent = jnp.dot(scaled, output_weight[...], preferred_element_type=jnp.float32)
        tangents[rows] = tangent.astype(jnp.bfloat16)
        ids = lax.broadcasted_iota(jnp.int32, (COLS_TILE, slots), 0) + start
        picks = jnp.where(named == ids, 1.0, 0.0).astype(jnp.bfloat16)
        if i == 0:
            copies[4].wait()
        gathered = jnp.dot(picks, cot[...], preferred_element_type=jnp.float32).astype(jnp.bfloat16)
        pulled = lax.dot_general(gathered, output_weight[...], ROWS_BY_COLS, preferred_element_type=jnp.float32)
        weighted = (slopes * pulled).astype(jnp.bfloat16)
        adjoint = lax.dot_general(weighted, hidden_weight[...], ROWS_BY_COLS, preferred_element_type=jnp.float32)
        if i == 0:
            copies[5].wait()
        base[rows] = base[rows] + adjoint
        outs.append(pltpu.make_async_copy(base.at[rows], base_out.at[rows], out_sems.at[i]))
        outs[-1].start()
    for out in outs:
        out.wait()


def network(count, columns, state, back, base, cot, hidden_weight, hidden_bias, output_weight):
    cols, levels = state.shape
    slots, chan = cot.shape
    hbm, vmem = pl.BlockSpec(memory_space=pltpu.HBM), pl.BlockSpec(memory_space=pltpu.VMEM)
    moved = (state, back, base, cot, hidden_weight, output_weight)
    return pl.pallas_call(
        network_kernel,
        in_specs=[pl.BlockSpec(memory_space=pltpu.SMEM), vmem, vmem] + [hbm] * 6,
        out_specs=[vmem, hbm, vmem],
        out_shape=[
            jax.ShapeDtypeStruct((cols, chan), jnp.bfloat16),
            jax.ShapeDtypeStruct((cols, levels), jnp.float32),
            TOKEN,
        ],
        scratch_shapes=[pltpu.VMEM(a.shape, a.dtype) for a in moved]
        + [pltpu.SemaphoreType.DMA((6,)), pltpu.SemaphoreType.DMA((cols // COLS_TILE,))],
        cost_estimate=pl.CostEstimate(
            flops=2 * (5 * cols + slots) * levels * hidden_bias.shape[1],
            bytes_accessed=12 << 20,
            transcendentals=1 << 20,
        ),
        compiler_params=pltpu.CompilerParams(vmem_limit_bytes=40 << 20),
        name="network",
    )(count, columns, hidden_bias, *in_hbm(*moved))


def spread_kernel(count, columns, tangents, _, out, held, sems):
    slots, cols = held.shape[0], tangents.shape[0]
    lane = lax.broadcasted_iota(jnp.int32, (LANES, LANES), 1)
    outs = []
    for i, start in enumerate(range(0, slots, SLOTS_TILE)):
        rows = slice(start, start + SLOTS_TILE)
        parts = []
        for s in range(start, start + SLOTS_TILE, LANES):
            alive = lax.broadcasted_iota(jnp.int32, (1, LANES), 1) + s < count[0]
            named = jnp.where(alive, columns[:, s : s + LANES], -1)
            mine = jnp.broadcast_to(named, (LANES, LANES)).T
            hits = [jnp.where(mine == lane + k, 1.0, 0.0).astype(jnp.bfloat16) for k in range(0, cols, LANES)]
            parts.append(jnp.concatenate(hits, axis=1))
        picks = jnp.concatenate(parts, axis=0)
        held[rows] = jnp.dot(picks, tangents[...], preferred_element_type=jnp.float32).astype(jnp.bfloat16)
        outs.append(pltpu.make_async_copy(held.at[rows], out.at[rows], sems.at[i]))
        outs[-1].start()
    for copy in outs:
        copy.wait()


def spread(count, columns, tangents, token):
    slots, (cols, chan) = columns.shape[1], tangents.shape
    vmem = pl.BlockSpec(memory_space=pltpu.VMEM)
    return pl.pallas_call(
        spread_kernel,
        in_specs=[pl.BlockSpec(memory_space=pltpu.SMEM), vmem, vmem, pl.BlockSpec(memory_space=pl.ANY)],
        out_specs=pl.BlockSpec(memory_space=pltpu.HBM),
        out_shape=jax.ShapeDtypeStruct((slots, chan), jnp.bfloat16),
        scratch_shapes=[
            pltpu.VMEM((slots, chan), jnp.bfloat16),
            pltpu.SemaphoreType.DMA((slots // SLOTS_TILE,)),
        ],
        compiler_params=pltpu.CompilerParams(vmem_limit_bytes=24 << 20),
        cost_estimate=pl.CostEstimate(flops=2 * slots * cols * chan, bytes_accessed=4 << 20, transcendentals=0),
        name="spread",
    )(count, columns, tangents, token)


def sent(array, to):
    counts = [lax.axis_size(axis) for axis in ("sub", "lat", "lon")]
    flat = lambda s, a, o: (s * counts[1] + a) * counts[2] + o
    pairs = []
    for s in range(counts[0]):
        for a in range(counts[1]):
            for o in range(counts[2]):
                target = to(s, a, o)
                if all(0 <= t < n for t, n in zip(target, counts)):
                    pairs.append((flat(s, a, o), flat(*target)))
    return lax.ppermute(array, ("sub", "lat", "lon"), pairs)


def local(
    increment,
    multiplier,
    background,
    obs_cotangent,
    obs_column,
    obs_count,
    transport,
    hidden_weight,
    hidden_bias,
    output_weight,
):
    increment, multiplier = increment[0], multiplier[0]
    levels = increment.shape[2]
    low, high, strip = pack(increment, multiplier)
    above = sent(high, lambda s, a, o: (s, a + 1, o))
    below = sent(low, lambda s, a, o: (s, a - 1, o))
    across = sent(strip, lambda s, a, o: (s, a, 1 - o))
    myself = lax.axis_index(("lat", "lon"))
    my_count = lax.dynamic_slice(obs_count[0], (myself,), (1,))
    tangents, base, token = network(
        my_count,
        obs_column[0],
        increment.reshape(-1, levels),
        background[0].reshape(-1, levels),
        multiplier.reshape(-1, levels),
        obs_cotangent[0, 0],
        hidden_weight,
        hidden_bias[None, :],
        output_weight,
    )
    low_corner, high_corner, token = corners(across, token)
    above_corner = sent(high_corner, lambda s, a, o: (s, a + 1, o))
    below_corner = sent(low_corner, lambda s, a, o: (s, a - 1, o))
    pieces = [above, below, across, above_corner, below_corner]
    crossing, token = transported(True, increment, multiplier, pieces, transport, token)
    from_chip = sent(crossing, lambda s, a, o: (s + 1 if s % 2 else s - 1, a, o))
    staying, token = transported(False, increment, multiplier, pieces, transport, token)
    from_core = sent(staying, lambda s, a, o: (s - 1 if s % 2 else s + 1, a, o))
    tangent = spread(my_count, obs_column[0], tangents, token)
    model_error, gradient = final(increment, base.reshape(increment.shape), from_chip, from_core)
    return (model_error[None], gradient[None], tangent[None, None])


def solution(mesh):
    in_specs = (
        P("sub", "lat", "lon", None),
        P("sub", "lat", "lon", None),
        P("sub", "lat", "lon", None),
        P("sub", ("lat", "lon"), None, None),
        P("sub", ("lat", "lon"), None),
        P("sub", None),
        P(),
        P(),
        P(),
        P(),
    )
    out_specs = (
        P("sub", "lat", "lon", None),
        P("sub", "lat", "lon", None),
        P("sub", ("lat", "lon"), None, None),
    )
    return jax.shard_map(local, mesh=mesh, in_specs=in_specs, out_specs=out_specs, check_vma=False)
```

```python
import functools

import jax
import jax.numpy as jnp
from jax import lax
from jax.experimental import pallas as pl
from jax.experimental.pallas import tpu as pltpu
from jax.sharding import PartitionSpec as P


STEPS = 4
REACH = 2 * STEPS
EDGE = REACH - 2
LANES = 128
COLS_TILE = 256
SLOTS_TILE = 512
PARTS = 2
MIRROR = (3, 2, 1, 0, 7, 6, 5, 4)
TOKEN = jax.ShapeDtypeStruct((8, LANES), jnp.float32)


CHUNK = 4


def in_hbm(*arrays):
    return [pltpu.with_memory_space_constraint(a, pltpu.HBM) for a in arrays]


def pack_kernel(inc, mul, low, high, strip, held, sems):
    lon = lax.axis_index("lon")
    rows, across = inc.shape[0], inc.shape[1]
    side = pl.multiple_of((across - REACH) * (1 - lon), REACH)
    copies = {}
    for start in range(0, rows, CHUNK):
        for f, src in enumerate((inc, mul)):
            part = pl.ds(start, CHUNK)
            copies[f, start] = pltpu.make_async_copy(src.at[part], held.at[f, part], sems.at[f, start // CHUNK])
            copies[f, start].start()
    for start in range(0, rows, CHUNK):
        for f in range(2):
            copies[f, start].wait()
            for r in range(start, start + CHUNK):
                row = held[f, r].astype(jnp.bfloat16)
                if r < REACH:
                    low[f, r] = row
                if r >= rows - REACH:
                    high[f, r - rows + REACH] = row
                strip[f, r] = held[f, r, pl.ds(side, REACH), :].astype(jnp.bfloat16)


def pack(increment, multiplier):
    rows, across, levels = increment.shape
    shapes = [(2, REACH, across), (2, REACH, across), (2, rows, REACH)]
    return pl.pallas_call(
        pack_kernel,
        in_specs=[pl.BlockSpec(memory_space=pltpu.HBM)] * 2,
        out_specs=[pl.BlockSpec(memory_space=pltpu.VMEM)] * 3,
        out_shape=[jax.ShapeDtypeStruct(s + (levels,), jnp.bfloat16) for s in shapes],
        scratch_shapes=[
            pltpu.VMEM((2,) + increment.shape, jnp.float32),
            pltpu.SemaphoreType.DMA((2, rows // CHUNK)),
        ],
        compiler_params=pltpu.CompilerParams(vmem_limit_bytes=16 << 20),
        name="pack",
    )(*in_hbm(increment, multiplier))


def corner_kernel(strip, _, low, high, token):
    rows = strip.shape[1]
    low[...] = strip[:, :EDGE]
    high[...] = strip[:, rows - EDGE :]
    token[...] = jnp.zeros_like(token)


def corners(strip, token):
    fields, _, wide, levels = strip.shape
    return pl.pallas_call(
        corner_kernel,
        in_specs=[pl.BlockSpec(memory_space=pltpu.VMEM), pl.BlockSpec(memory_space=pl.ANY)],
        out_shape=[jax.ShapeDtypeStruct((fields, EDGE, wide, levels), jnp.bfloat16)] * 2 + [TOKEN],
        compiler_params=pltpu.CompilerParams(vmem_limit_bytes=8 << 20),
        name="corners",
    )(strip, token)


def sweep(src, dst, taps, first, last, blocks):
    c0, c1, c2, c3, c4, c5, c6, c7 = taps
    group = 4
    for i in range(first, last, group):
        for b in range(blocks):
            j = 8 + 8 * b
            at = [src[i - 2 + r, j : j + 8, :] for r in range(group + 4)]
            for r in range(group):
                total = at[r + 2] + c0 * at[r]
                total = total + c1 * at[r + 1]
                total = total + c2 * at[r + 3]
                total = total + c3 * at[r + 4]
                total = total + c4 * src[i + r, j - 2 : j + 6, :]
                total = total + c5 * src[i + r, j - 1 : j + 7, :]
                total = total + c6 * src[i + r, j + 1 : j + 9, :]
                total = total + c7 * src[i + r, j + 2 : j + 10, :]
                dst[i + r, j : j + 8, :] = total


def transport_kernel(
    crossing, low_tile, inc, mul, above, below, strip, above_corner, below_corner, rates, _, out, token, bufs, other, sems
):
    lat, lon = lax.axis_index("lat"), lax.axis_index("lon")
    odd = lax.rem(lax.axis_index("sub"), 2)
    n_lat = lax.axis_size("lat")
    rows, across = inc.shape[0], inc.shape[1]
    tall = rows + 2 * REACH
    blocks = (across + REACH) // 8
    tiles = bufs.shape[0]
    own = pl.multiple_of(8 + REACH * lon, 8)
    beside = pl.multiple_of(8 + across * (1 - lon), 8)
    f = 1 - odd if crossing else odd
    forward = f == 0

    def arriving(src, t):
        there = bufs.at[t, pl.ds(REACH, rows), pl.ds(own, across), :]
        return pltpu.make_async_copy(src.at[:, :, pl.ds((low_tile + t) * LANES, LANES)], there, sems.at[t])

    @pl.when(forward)
    def _():
        for t in range(tiles):
            arriving(inc, t).start()

    @pl.when(jnp.logical_not(forward))
    def _():
        for t in range(tiles):
            arriving(mul, t).start()

    token[...] = jnp.zeros_like(token)
    blank = jnp.zeros((8, LANES), jnp.float32)
    for r in range(tall):
        other[r] = jnp.zeros(other.shape[1:], jnp.float32)
        for t in range(tiles):
            bufs[t, r, 0:8, :] = blank
            bufs[t, r, 8 * blocks + 8 : 8 * blocks + 16, :] = blank
    for t in range(tiles):
        for r in (0, 1, tall - 2, tall - 1):
            bufs[t, r, pl.ds(beside, REACH), :] = blank
        for r in range(REACH):
            lanes = slice((low_tile + t) * LANES, (low_tile + t + 1) * LANES)
            bufs[t, r, pl.ds(own, across), :] = above[f, r, :, lanes].astype(jnp.float32)
            bufs[t, rows + REACH + r, pl.ds(own, across), :] = below[f, r, :, lanes].astype(jnp.float32)
        for r in range(rows):
            bufs[t, REACH + r, pl.ds(beside, REACH), :] = strip[f, r, :, lanes].astype(jnp.float32)
        for r in range(EDGE):
            bufs[t, REACH - EDGE + r, pl.ds(beside, REACH), :] = above_corner[f, r, :, lanes].astype(jnp.float32)
            bufs[t, rows + REACH + r, pl.ds(beside, REACH), :] = below_corner[f, r, :, lanes].astype(jnp.float32)

    def tile_of(t, carry):
        lanes = pl.ds(pl.multiple_of((low_tile + t) * LANES, LANES), LANES)
        out_lanes = pl.ds(pl.multiple_of(t * LANES, LANES), LANES)
        pltpu.make_async_copy(
            inc.at[:, :, lanes], bufs.at[t, pl.ds(REACH, rows), pl.ds(own, across), :], sems.at[t]
        ).wait()
        spread = [
            jnp.broadcast_to(jnp.where(forward, rates[k : k + 1, lanes], rates[m : m + 1, lanes]), (8, LANES))
            for k, m in enumerate(MIRROR)
        ]
        rest = spread[0]
        for k in range(1, 8):
            rest = rest + spread[k]
        center = 1.0 - rest
        taps = [c / center for c in spread]
        scale = (center * center) * (center * center)
        a, b = bufs.at[t], other
        for step in range(STEPS):
            first, last = 2 * (step + 1), tall - 2 * (step + 1)
            sweep(a, b, taps, first, last, blocks)
            if step < STEPS - 1:

                @pl.when(lat == 0)
                def _(b=b, first=first):
                    for r in range(first, REACH):
                        b[r] = jnp.zeros(b.shape[1:], jnp.float32)

                @pl.when(lat == n_lat - 1)
                def _(b=b, last=last):
                    for r in range(rows + REACH, last):
                        b[r] = jnp.zeros(b.shape[1:], jnp.float32)

            a, b = b, a
        for r in range(rows):
            out[r, :, out_lanes] = (scale[0:1] * a[REACH + r, pl.ds(own, across), :]).astype(jnp.bfloat16)
        return carry

    lax.fori_loop(0, tiles, tile_of, 0)


def transported(crossing, low_tile, tiles, increment, multiplier, pieces, rates, token):
    rows, across, _ = increment.shape
    tall, wide = rows + 2 * REACH, across + REACH + 16
    hbm, vmem = pl.BlockSpec(memory_space=pltpu.HBM), pl.BlockSpec(memory_space=pltpu.VMEM)
    return pl.pallas_call(
        functools.partial(transport_kernel, crossing, low_tile),
        in_specs=[hbm, hbm] + [vmem] * (len(pieces) + 1) + [pl.BlockSpec(memory_space=pl.ANY)],
        out_specs=[vmem, vmem],
        out_shape=[jax.ShapeDtypeStruct((rows, across, tiles * LANES), jnp.bfloat16), TOKEN],
        scratch_shapes=[
            pltpu.VMEM((tiles, tall, wide, LANES), jnp.float32),
            pltpu.VMEM((tall, wide, LANES), jnp.float32),
            pltpu.SemaphoreType.DMA((tiles,)),
        ],
        compiler_params=pltpu.CompilerParams(vmem_limit_bytes=24 << 20),
        cost_estimate=pl.CostEstimate(flops=12_500_000 * tiles, bytes_accessed=tiles << 20, transcendentals=0),
        name="crossing" if crossing else "staying",
    )(*in_hbm(increment, multiplier), *pieces, rates, token)


def final_kernel(inc, base, from_core, *refs):
    odd = lax.rem(lax.axis_index("sub"), 2) == 1
    from_chip, (error_out, grad_out) = refs[:-2], refs[-2:]
    width = from_chip[0].shape[2]
    group = 2
    for r in range(0, inc.shape[0], group):
        rows = slice(r, r + group)
        for part, ref in enumerate(from_chip):
            lanes = slice(part * width, (part + 1) * width)
            x = ref[rows].astype(jnp.float32)
            d = from_core[rows, :, lanes].astype(jnp.float32)
            error_out[rows, :, lanes] = inc[rows, :, lanes] - jnp.where(odd, d, x)
            grad_out[rows, :, lanes] = base[rows, :, lanes] - jnp.where(odd, x, d)


def final(increment, base, from_core, from_chip):
    rows, across, levels = increment.shape
    block = pl.BlockSpec((4, across, levels), lambda i: (i, 0, 0))
    part = pl.BlockSpec((4, across, levels // len(from_chip)), lambda i: (i, 0, 0))
    return pl.pallas_call(
        final_kernel,
        grid=(rows // 4,),
        in_specs=[block] * 3 + [part] * len(from_chip),
        out_specs=[block] * 2,
        out_shape=[jax.ShapeDtypeStruct(increment.shape, jnp.float32)] * 2,
        compiler_params=pltpu.CompilerParams(vmem_limit_bytes=16 << 20),
        cost_estimate=pl.CostEstimate(flops=4_000_000, bytes_accessed=10 << 20, transcendentals=0),
        name="final",
    )(increment, base, from_core, *from_chip)


ROWS_BY_COLS = (((1,), (1,)), ((), ()))


def network_kernel(
    count, columns, hidden_bias, state_in, back_in, base_in, cot_in, hidden_in, output_in,
    tangents, base_out, token,
    state, back, base, cot, hidden_weight, output_weight, sems, out_sems,
):
    cols, slots = state.shape[0], cot.shape[0]
    moves = [
        (hidden_in, hidden_weight), (back_in, back), (state_in, state),
        (output_in, output_weight), (cot_in, cot), (base_in, base),
    ]
    copies = [pltpu.make_async_copy(a, b, sems.at[i]) for i, (a, b) in enumerate(moves)]
    for copy in copies:
        copy.start()
    token[...] = jnp.zeros_like(token)
    alive = lax.broadcasted_iota(jnp.int32, (1, slots), 1) < count[0]
    named = jnp.where(alive, columns[...], -1)
    outs = []
    for i, start in enumerate(range(0, cols, COLS_TILE)):
        rows = slice(start, start + COLS_TILE)
        if i == 0:
            copies[0].wait()
            copies[1].wait()
        preact = jnp.dot(back[rows], hidden_weight[...], preferred_element_type=jnp.float32) + hidden_bias[...]
        hidden = jnp.tanh(preact)
        slopes = 1.0 - hidden * hidden
        if i == 0:
            copies[2].wait()
        forward = jnp.dot(state[rows].astype(jnp.bfloat16), hidden_weight[...], preferred_element_type=jnp.float32)
        scaled = (slopes * forward).astype(jnp.bfloat16)
        if i == 0:
            copies[3].wait()
        tangent = jnp.dot(scaled, output_weight[...], preferred_element_type=jnp.float32)
        tangents[rows] = tangent.astype(jnp.bfloat16)
        ids = lax.broadcasted_iota(jnp.int32, (COLS_TILE, slots), 0) + start
        picks = jnp.where(named == ids, 1.0, 0.0).astype(jnp.bfloat16)
        if i == 0:
            copies[4].wait()
        gathered = jnp.dot(picks, cot[...], preferred_element_type=jnp.float32).astype(jnp.bfloat16)
        pulled = lax.dot_general(gathered, output_weight[...], ROWS_BY_COLS, preferred_element_type=jnp.float32)
        weighted = (slopes * pulled).astype(jnp.bfloat16)
        adjoint = lax.dot_general(weighted, hidden_weight[...], ROWS_BY_COLS, preferred_element_type=jnp.float32)
        if i == 0:
            copies[5].wait()
        base[rows] = base[rows] + adjoint
        outs.append(pltpu.make_async_copy(base.at[rows], base_out.at[rows], out_sems.at[i]))
        outs[-1].start()
    for out in outs:
        out.wait()


def network(count, columns, state, back, base, cot, hidden_weight, hidden_bias, output_weight):
    cols, levels = state.shape
    slots, chan = cot.shape
    hbm, vmem = pl.BlockSpec(memory_space=pltpu.HBM), pl.BlockSpec(memory_space=pltpu.VMEM)
    moved = (state, back, base, cot, hidden_weight, output_weight)
    return pl.pallas_call(
        network_kernel,
        in_specs=[pl.BlockSpec(memory_space=pltpu.SMEM), vmem, vmem] + [hbm] * 6,
        out_specs=[vmem, hbm, vmem],
        out_shape=[
            jax.ShapeDtypeStruct((cols, chan), jnp.bfloat16),
            jax.ShapeDtypeStruct((cols, levels), jnp.float32),
            TOKEN,
        ],
        scratch_shapes=[pltpu.VMEM(a.shape, a.dtype) for a in moved]
        + [pltpu.SemaphoreType.DMA((6,)), pltpu.SemaphoreType.DMA((cols // COLS_TILE,))],
        cost_estimate=pl.CostEstimate(
            flops=2 * (5 * cols + slots) * levels * hidden_bias.shape[1],
            bytes_accessed=12 << 20,
            transcendentals=1 << 20,
        ),
        compiler_params=pltpu.CompilerParams(vmem_limit_bytes=40 << 20),
        name="network",
    )(count, columns, hidden_bias, *in_hbm(*moved))


def spread_kernel(count, columns, tangents, _, out, token, held, sems):
    slots, cols = held.shape[0], tangents.shape[0]
    token[...] = jnp.zeros_like(token)
    lane = lax.broadcasted_iota(jnp.int32, (LANES, LANES), 1)
    outs = []
    for i, start in enumerate(range(0, slots, SLOTS_TILE)):
        rows = slice(start, start + SLOTS_TILE)
        parts = []
        for s in range(start, start + SLOTS_TILE, LANES):
            alive = lax.broadcasted_iota(jnp.int32, (1, LANES), 1) + s < count[0]
            named = jnp.where(alive, columns[:, s : s + LANES], -1)
            mine = jnp.broadcast_to(named, (LANES, LANES)).T
            hits = [jnp.where(mine == lane + k, 1.0, 0.0).astype(jnp.bfloat16) for k in range(0, cols, LANES)]
            parts.append(jnp.concatenate(hits, axis=1))
        picks = jnp.concatenate(parts, axis=0)
        held[rows] = jnp.dot(picks, tangents[...], preferred_element_type=jnp.float32).astype(jnp.bfloat16)
        outs.append(pltpu.make_async_copy(held.at[rows], out.at[rows], sems.at[i]))
        outs[-1].start()
    for copy in outs:
        copy.wait()


def spread(count, columns, tangents, token):
    slots, (cols, chan) = columns.shape[1], tangents.shape
    vmem = pl.BlockSpec(memory_space=pltpu.VMEM)
    return pl.pallas_call(
        spread_kernel,
        in_specs=[pl.BlockSpec(memory_space=pltpu.SMEM), vmem, vmem, pl.BlockSpec(memory_space=pl.ANY)],
        out_specs=[pl.BlockSpec(memory_space=pltpu.HBM), vmem],
        out_shape=[jax.ShapeDtypeStruct((slots, chan), jnp.bfloat16), TOKEN],
        scratch_shapes=[
            pltpu.VMEM((slots, chan), jnp.bfloat16),
            pltpu.SemaphoreType.DMA((slots // SLOTS_TILE,)),
        ],
        compiler_params=pltpu.CompilerParams(vmem_limit_bytes=24 << 20),
        cost_estimate=pl.CostEstimate(flops=2 * slots * cols * chan, bytes_accessed=4 << 20, transcendentals=0),
        name="spread",
    )(count, columns, tangents, token)


def sent(array, to):
    counts = [lax.axis_size(axis) for axis in ("sub", "lat", "lon")]
    flat = lambda s, a, o: (s * counts[1] + a) * counts[2] + o
    pairs = []
    for s in range(counts[0]):
        for a in range(counts[1]):
            for o in range(counts[2]):
                target = to(s, a, o)
                if all(0 <= t < n for t, n in zip(target, counts)):
                    pairs.append((flat(s, a, o), flat(*target)))
    return lax.ppermute(array, ("sub", "lat", "lon"), pairs)


def local(
    increment,
    multiplier,
    background,
    obs_cotangent,
    obs_column,
    obs_count,
    transport,
    hidden_weight,
    hidden_bias,
    output_weight,
):
    increment, multiplier = increment[0], multiplier[0]
    levels = increment.shape[2]
    low, high, strip = pack(increment, multiplier)
    above = sent(high, lambda s, a, o: (s, a + 1, o))
    below = sent(low, lambda s, a, o: (s, a - 1, o))
    across = sent(strip, lambda s, a, o: (s, a, 1 - o))
    myself = lax.axis_index(("lat", "lon"))
    my_count = lax.dynamic_slice(obs_count[0], (myself,), (1,))
    tangents, base, token = network(
        my_count,
        obs_column[0],
        increment.reshape(-1, levels),
        background[0].reshape(-1, levels),
        multiplier.reshape(-1, levels),
        obs_cotangent[0, 0],
        hidden_weight,
        hidden_bias[None, :],
        output_weight,
    )
    low_corner, high_corner, token = corners(across, token)
    above_corner = sent(high_corner, lambda s, a, o: (s, a + 1, o))
    below_corner = sent(low_corner, lambda s, a, o: (s, a - 1, o))
    pieces = [above, below, across, above_corner, below_corner]
    tangent, token = spread(my_count, obs_column[0], tangents, token)
    tiles = levels // LANES
    from_chip = []
    for part in range(PARTS):
        crossing, token = transported(
            True, part * tiles // PARTS, tiles // PARTS, increment, multiplier, pieces, transport, token
        )
        from_chip.append(sent(crossing, lambda s, a, o: (s + 1 if s % 2 else s - 1, a, o)))
    staying, _ = transported(False, 0, tiles, increment, multiplier, pieces, transport, token)
    from_core = sent(staying, lambda s, a, o: (s - 1 if s % 2 else s + 1, a, o))
    model_error, gradient = final(increment, base.reshape(increment.shape), from_core, from_chip)
    return (model_error[None], gradient[None], tangent[None, None])


def solution(mesh):
    in_specs = (
        P("sub", "lat", "lon", None),
        P("sub", "lat", "lon", None),
        P("sub", "lat", "lon", None),
        P("sub", ("lat", "lon"), None, None),
        P("sub", ("lat", "lon"), None),
        P("sub", None),
        P(),
        P(),
        P(),
        P(),
    )
    out_specs = (
        P("sub", "lat", "lon", None),
        P("sub", "lat", "lon", None),
        P("sub", ("lat", "lon"), None, None),
    )
    return jax.shard_map(local, mesh=mesh, in_specs=in_specs, out_specs=out_specs, check_vma=False)
```

```python
import functools

import jax
import jax.numpy as jnp
from jax import lax
from jax.experimental import pallas as pl
from jax.experimental.pallas import tpu as pltpu
from jax.sharding import PartitionSpec as P


STEPS = 4
REACH = 2 * STEPS
EDGE = REACH - 2
LANES = 128
COLS_TILE = 256
SLOTS_TILE = 512
MIRROR = (3, 2, 1, 0, 7, 6, 5, 4)
TOKEN = jax.ShapeDtypeStruct((8, LANES), jnp.float32)


CHUNK = 4


def in_hbm(*arrays):
    return [pltpu.with_memory_space_constraint(a, pltpu.HBM) for a in arrays]


def pack_kernel(inc, mul, low, high, strip, held, sems):
    lon = lax.axis_index("lon")
    rows, across = inc.shape[0], inc.shape[1]
    side = pl.multiple_of((across - REACH) * (1 - lon), REACH)
    copies = {}
    for start in range(0, rows, CHUNK):
        for f, src in enumerate((inc, mul)):
            part = pl.ds(start, CHUNK)
            copies[f, start] = pltpu.make_async_copy(src.at[part], held.at[f, part], sems.at[f, start // CHUNK])
            copies[f, start].start()
    for start in range(0, rows, CHUNK):
        for f in range(2):
            copies[f, start].wait()
            for r in range(start, start + CHUNK):
                row = held[f, r].astype(jnp.bfloat16)
                if r < REACH:
                    low[f, r] = row
                if r >= rows - REACH:
                    high[f, r - rows + REACH] = row
                strip[f, r] = held[f, r, pl.ds(side, REACH), :].astype(jnp.bfloat16)


def pack(increment, multiplier):
    rows, across, levels = increment.shape
    shapes = [(2, REACH, across), (2, REACH, across), (2, rows, REACH)]
    return pl.pallas_call(
        pack_kernel,
        in_specs=[pl.BlockSpec(memory_space=pltpu.HBM)] * 2,
        out_specs=[pl.BlockSpec(memory_space=pltpu.VMEM)] * 3,
        out_shape=[jax.ShapeDtypeStruct(s + (levels,), jnp.bfloat16) for s in shapes],
        scratch_shapes=[
            pltpu.VMEM((2,) + increment.shape, jnp.float32),
            pltpu.SemaphoreType.DMA((2, rows // CHUNK)),
        ],
        compiler_params=pltpu.CompilerParams(vmem_limit_bytes=16 << 20),
        name="pack",
    )(*in_hbm(increment, multiplier))


def corner_kernel(strip, _, low, high, token):
    rows = strip.shape[1]
    low[...] = strip[:, :EDGE]
    high[...] = strip[:, rows - EDGE :]
    token[...] = jnp.zeros_like(token)


def corners(strip, token):
    fields, _, wide, levels = strip.shape
    return pl.pallas_call(
        corner_kernel,
        in_specs=[pl.BlockSpec(memory_space=pltpu.VMEM), pl.BlockSpec(memory_space=pl.ANY)],
        out_shape=[jax.ShapeDtypeStruct((fields, EDGE, wide, levels), jnp.bfloat16)] * 2 + [TOKEN],
        compiler_params=pltpu.CompilerParams(vmem_limit_bytes=8 << 20),
        name="corners",
    )(strip, token)


def sweep(src, dst, taps, first, last, blocks):
    c0, c1, c2, c3, c4, c5, c6, c7 = taps
    group = 4
    for i in range(first, last, group):
        for b in range(blocks):
            j = 8 + 8 * b
            at = [src[i - 2 + r, j : j + 8, :] for r in range(group + 4)]
            for r in range(group):
                total = at[r + 2] + c0 * at[r]
                total = total + c1 * at[r + 1]
                total = total + c2 * at[r + 3]
                total = total + c3 * at[r + 4]
                total = total + c4 * src[i + r, j - 2 : j + 6, :]
                total = total + c5 * src[i + r, j - 1 : j + 7, :]
                total = total + c6 * src[i + r, j + 1 : j + 9, :]
                total = total + c7 * src[i + r, j + 2 : j + 10, :]
                dst[i + r, j : j + 8, :] = total


def transport_kernel(
    crossing, low_tile, inc, mul, above, below, strip, above_corner, below_corner, rates, _, out, token, bufs, other, sems
):
    lat, lon = lax.axis_index("lat"), lax.axis_index("lon")
    odd = lax.rem(lax.axis_index("sub"), 2)
    n_lat = lax.axis_size("lat")
    rows, across = inc.shape[0], inc.shape[1]
    tall = rows + 2 * REACH
    blocks = (across + REACH) // 8
    tiles = bufs.shape[0]
    own = pl.multiple_of(8 + REACH * lon, 8)
    beside = pl.multiple_of(8 + across * (1 - lon), 8)
    f = 1 - odd if crossing else odd
    forward = f == 0

    def arriving(src, t):
        there = bufs.at[t, pl.ds(REACH, rows), pl.ds(own, across), :]
        return pltpu.make_async_copy(src.at[:, :, pl.ds((low_tile + t) * LANES, LANES)], there, sems.at[t])

    @pl.when(forward)
    def _():
        for t in range(tiles):
            arriving(inc, t).start()

    @pl.when(jnp.logical_not(forward))
    def _():
        for t in range(tiles):
            arriving(mul, t).start()

    token[...] = jnp.zeros_like(token)
    blank = jnp.zeros((8, LANES), jnp.float32)
    for r in range(tall):
        other[r] = jnp.zeros(other.shape[1:], jnp.float32)
        for t in range(tiles):
            bufs[t, r, 0:8, :] = blank
            bufs[t, r, 8 * blocks + 8 : 8 * blocks + 16, :] = blank
    for t in range(tiles):
        for r in (0, 1, tall - 2, tall - 1):
            bufs[t, r, pl.ds(beside, REACH), :] = blank
        for r in range(REACH):
            lanes = slice((low_tile + t) * LANES, (low_tile + t + 1) * LANES)
            bufs[t, r, pl.ds(own, across), :] = above[f, r, :, lanes].astype(jnp.float32)
            bufs[t, rows + REACH + r, pl.ds(own, across), :] = below[f, r, :, lanes].astype(jnp.float32)
        for r in range(rows):
            bufs[t, REACH + r, pl.ds(beside, REACH), :] = strip[f, r, :, lanes].astype(jnp.float32)
        for r in range(EDGE):
            bufs[t, REACH - EDGE + r, pl.ds(beside, REACH), :] = above_corner[f, r, :, lanes].astype(jnp.float32)
            bufs[t, rows + REACH + r, pl.ds(beside, REACH), :] = below_corner[f, r, :, lanes].astype(jnp.float32)

    def tile_of(t, carry):
        lanes = pl.ds(pl.multiple_of((low_tile + t) * LANES, LANES), LANES)
        out_lanes = pl.ds(pl.multiple_of(t * LANES, LANES), LANES)
        pltpu.make_async_copy(
            inc.at[:, :, lanes], bufs.at[t, pl.ds(REACH, rows), pl.ds(own, across), :], sems.at[t]
        ).wait()
        spread = [
            jnp.broadcast_to(jnp.where(forward, rates[k : k + 1, lanes], rates[m : m + 1, lanes]), (8, LANES))
            for k, m in enumerate(MIRROR)
        ]
        rest = spread[0]
        for k in range(1, 8):
            rest = rest + spread[k]
        center = 1.0 - rest
        taps = [c / center for c in spread]
        scale = (center * center) * (center * center)
        a, b = bufs.at[t], other
        for step in range(STEPS):
            first, last = 2 * (step + 1), tall - 2 * (step + 1)
            sweep(a, b, taps, first, last, blocks)
            if step < STEPS - 1:

                @pl.when(lat == 0)
                def _(b=b, first=first):
                    for r in range(first, REACH):
                        b[r] = jnp.zeros(b.shape[1:], jnp.float32)

                @pl.when(lat == n_lat - 1)
                def _(b=b, last=last):
                    for r in range(rows + REACH, last):
                        b[r] = jnp.zeros(b.shape[1:], jnp.float32)

            a, b = b, a
        for r in range(rows):
            out[r, :, out_lanes] = (scale[0:1] * a[REACH + r, pl.ds(own, across), :]).astype(jnp.bfloat16)
        return carry

    lax.fori_loop(0, tiles, tile_of, 0)


def transported(crossing, low_tile, tiles, increment, multiplier, pieces, rates, token):
    rows, across, _ = increment.shape
    tall, wide = rows + 2 * REACH, across + REACH + 16
    hbm, vmem = pl.BlockSpec(memory_space=pltpu.HBM), pl.BlockSpec(memory_space=pltpu.VMEM)
    return pl.pallas_call(
        functools.partial(transport_kernel, crossing, low_tile),
        in_specs=[hbm, hbm] + [vmem] * (len(pieces) + 1) + [pl.BlockSpec(memory_space=pl.ANY)],
        out_specs=[vmem, vmem],
        out_shape=[jax.ShapeDtypeStruct((rows, across, tiles * LANES), jnp.bfloat16), TOKEN],
        scratch_shapes=[
            pltpu.VMEM((tiles, tall, wide, LANES), jnp.float32),
            pltpu.VMEM((tall, wide, LANES), jnp.float32),
            pltpu.SemaphoreType.DMA((tiles,)),
        ],
        compiler_params=pltpu.CompilerParams(vmem_limit_bytes=24 << 20),
        cost_estimate=pl.CostEstimate(flops=12_500_000 * tiles, bytes_accessed=tiles << 20, transcendentals=0),
        name="crossing" if crossing else "staying",
    )(*in_hbm(increment, multiplier), *pieces, rates, token)


def final_kernel(inc, base, from_chip, from_core, error_out, grad_out, error, grad, sems):
    odd = lax.rem(lax.axis_index("sub"), 2) == 1
    copies = []
    for start in range(0, inc.shape[0], CHUNK):
        for r in range(start, start + CHUNK):
            x = from_chip[r].astype(jnp.float32)
            d = from_core[r].astype(jnp.float32)
            error[r] = inc[r] - jnp.where(odd, d, x)
            grad[r] = base[r] - jnp.where(odd, x, d)
        rows = pl.ds(start, CHUNK)
        for f, (held, out) in enumerate(((error, error_out), (grad, grad_out))):
            copies.append(pltpu.make_async_copy(held.at[rows], out.at[rows], sems.at[f, start // CHUNK]))
            copies[-1].start()
    for copy in copies:
        copy.wait()


def final(increment, base, from_chip, from_core):
    hbm, vmem = pl.BlockSpec(memory_space=pltpu.HBM), pl.BlockSpec(memory_space=pltpu.VMEM)
    return pl.pallas_call(
        final_kernel,
        in_specs=[vmem] * 4,
        out_specs=[hbm] * 2,
        out_shape=[jax.ShapeDtypeStruct(increment.shape, jnp.float32)] * 2,
        scratch_shapes=[pltpu.VMEM(increment.shape, jnp.float32)] * 2
        + [pltpu.SemaphoreType.DMA((2, increment.shape[0] // CHUNK))],
        compiler_params=pltpu.CompilerParams(vmem_limit_bytes=16 << 20),
        cost_estimate=pl.CostEstimate(flops=4_000_000, bytes_accessed=10 << 20, transcendentals=0),
        name="final",
    )(increment, base, from_chip, from_core)


ROWS_BY_COLS = (((1,), (1,)), ((), ()))


def network_kernel(
    count, columns, hidden_bias, state_in, back_in, base_in, cot_in, hidden_in, output_in,
    tangents, base_out, token,
    state, back, base, cot, hidden_weight, output_weight, sems, out_sems,
):
    cols, slots = state.shape[0], cot.shape[0]
    moves = [
        (hidden_in, hidden_weight), (back_in, back), (state_in, state),
        (output_in, output_weight), (cot_in, cot), (base_in, base),
    ]
    copies = [pltpu.make_async_copy(a, b, sems.at[i]) for i, (a, b) in enumerate(moves)]
    for copy in copies:
        copy.start()
    token[...] = jnp.zeros_like(token)
    alive = lax.broadcasted_iota(jnp.int32, (1, slots), 1) < count[0]
    named = jnp.where(alive, columns[...], -1)
    outs = []
    for i, start in enumerate(range(0, cols, COLS_TILE)):
        rows = slice(start, start + COLS_TILE)
        if i == 0:
            copies[0].wait()
            copies[1].wait()
        preact = jnp.dot(back[rows], hidden_weight[...], preferred_element_type=jnp.float32) + hidden_bias[...]
        hidden = jnp.tanh(preact)
        slopes = 1.0 - hidden * hidden
        if i == 0:
            copies[2].wait()
        forward = jnp.dot(state[rows].astype(jnp.bfloat16), hidden_weight[...], preferred_element_type=jnp.float32)
        scaled = (slopes * forward).astype(jnp.bfloat16)
        if i == 0:
            copies[3].wait()
        tangent = jnp.dot(scaled, output_weight[...], preferred_element_type=jnp.float32)
        tangents[rows] = tangent.astype(jnp.bfloat16)
        ids = lax.broadcasted_iota(jnp.int32, (COLS_TILE, slots), 0) + start
        picks = jnp.where(named == ids, 1.0, 0.0).astype(jnp.bfloat16)
        if i == 0:
            copies[4].wait()
        gathered = jnp.dot(picks, cot[...], preferred_element_type=jnp.float32).astype(jnp.bfloat16)
        pulled = lax.dot_general(gathered, output_weight[...], ROWS_BY_COLS, preferred_element_type=jnp.float32)
        weighted = (slopes * pulled).astype(jnp.bfloat16)
        adjoint = lax.dot_general(weighted, hidden_weight[...], ROWS_BY_COLS, preferred_element_type=jnp.float32)
        if i == 0:
            copies[5].wait()
        base[rows] = base[rows] + adjoint
        outs.append(pltpu.make_async_copy(base.at[rows], base_out.at[rows], out_sems.at[i]))
        outs[-1].start()
    for out in outs:
        out.wait()


def network(count, columns, state, back, base, cot, hidden_weight, hidden_bias, output_weight):
    cols, levels = state.shape
    slots, chan = cot.shape
    hbm, vmem = pl.BlockSpec(memory_space=pltpu.HBM), pl.BlockSpec(memory_space=pltpu.VMEM)
    moved = (state, back, base, cot, hidden_weight, output_weight)
    return pl.pallas_call(
        network_kernel,
        in_specs=[pl.BlockSpec(memory_space=pltpu.SMEM), vmem, vmem] + [hbm] * 6,
        out_specs=[vmem, hbm, vmem],
        out_shape=[
            jax.ShapeDtypeStruct((cols, chan), jnp.bfloat16),
            jax.ShapeDtypeStruct((cols, levels), jnp.float32),
            TOKEN,
        ],
        scratch_shapes=[pltpu.VMEM(a.shape, a.dtype) for a in moved]
        + [pltpu.SemaphoreType.DMA((6,)), pltpu.SemaphoreType.DMA((cols // COLS_TILE,))],
        cost_estimate=pl.CostEstimate(
            flops=2 * (5 * cols + slots) * levels * hidden_bias.shape[1],
            bytes_accessed=12 << 20,
            transcendentals=1 << 20,
        ),
        compiler_params=pltpu.CompilerParams(vmem_limit_bytes=40 << 20),
        name="network",
    )(count, columns, hidden_bias, *in_hbm(*moved))


def spread_kernel(count, columns, tangents, _, out, token, held, sems):
    slots, cols = held.shape[0], tangents.shape[0]
    token[...] = jnp.zeros_like(token)
    lane = lax.broadcasted_iota(jnp.int32, (LANES, LANES), 1)
    outs = []
    for i, start in enumerate(range(0, slots, SLOTS_TILE)):
        rows = slice(start, start + SLOTS_TILE)
        parts = []
        for s in range(start, start + SLOTS_TILE, LANES):
            alive = lax.broadcasted_iota(jnp.int32, (1, LANES), 1) + s < count[0]
            named = jnp.where(alive, columns[:, s : s + LANES], -1)
            mine = jnp.broadcast_to(named, (LANES, LANES)).T
            hits = [jnp.where(mine == lane + k, 1.0, 0.0).astype(jnp.bfloat16) for k in range(0, cols, LANES)]
            parts.append(jnp.concatenate(hits, axis=1))
        picks = jnp.concatenate(parts, axis=0)
        held[rows] = jnp.dot(picks, tangents[...], preferred_element_type=jnp.float32).astype(jnp.bfloat16)
        outs.append(pltpu.make_async_copy(held.at[rows], out.at[rows], sems.at[i]))
        outs[-1].start()
    for copy in outs:
        copy.wait()


def spread(count, columns, tangents, token):
    slots, (cols, chan) = columns.shape[1], tangents.shape
    vmem = pl.BlockSpec(memory_space=pltpu.VMEM)
    return pl.pallas_call(
        spread_kernel,
        in_specs=[pl.BlockSpec(memory_space=pltpu.SMEM), vmem, vmem, pl.BlockSpec(memory_space=pl.ANY)],
        out_specs=[pl.BlockSpec(memory_space=pltpu.HBM), vmem],
        out_shape=[jax.ShapeDtypeStruct((slots, chan), jnp.bfloat16), TOKEN],
        scratch_shapes=[
            pltpu.VMEM((slots, chan), jnp.bfloat16),
            pltpu.SemaphoreType.DMA((slots // SLOTS_TILE,)),
        ],
        compiler_params=pltpu.CompilerParams(vmem_limit_bytes=24 << 20),
        cost_estimate=pl.CostEstimate(flops=2 * slots * cols * chan, bytes_accessed=4 << 20, transcendentals=0),
        name="spread",
    )(count, columns, tangents, token)


def sent(array, to):
    counts = [lax.axis_size(axis) for axis in ("sub", "lat", "lon")]
    flat = lambda s, a, o: (s * counts[1] + a) * counts[2] + o
    pairs = []
    for s in range(counts[0]):
        for a in range(counts[1]):
            for o in range(counts[2]):
                target = to(s, a, o)
                if all(0 <= t < n for t, n in zip(target, counts)):
                    pairs.append((flat(s, a, o), flat(*target)))
    return lax.ppermute(array, ("sub", "lat", "lon"), pairs)


def local(
    increment,
    multiplier,
    background,
    obs_cotangent,
    obs_column,
    obs_count,
    transport,
    hidden_weight,
    hidden_bias,
    output_weight,
):
    increment, multiplier = increment[0], multiplier[0]
    levels = increment.shape[2]
    low, high, strip = pack(increment, multiplier)
    above = sent(high, lambda s, a, o: (s, a + 1, o))
    below = sent(low, lambda s, a, o: (s, a - 1, o))
    across = sent(strip, lambda s, a, o: (s, a, 1 - o))
    myself = lax.axis_index(("lat", "lon"))
    my_count = lax.dynamic_slice(obs_count[0], (myself,), (1,))
    tangents, base, token = network(
        my_count,
        obs_column[0],
        increment.reshape(-1, levels),
        background[0].reshape(-1, levels),
        multiplier.reshape(-1, levels),
        obs_cotangent[0, 0],
        hidden_weight,
        hidden_bias[None, :],
        output_weight,
    )
    low_corner, high_corner, token = corners(across, token)
    above_corner = sent(high_corner, lambda s, a, o: (s, a + 1, o))
    below_corner = sent(low_corner, lambda s, a, o: (s, a - 1, o))
    pieces = [above, below, across, above_corner, below_corner]
    tangent, token = spread(my_count, obs_column[0], tangents, token)
    tiles = levels // LANES
    crossing, token = transported(True, 0, tiles, increment, multiplier, pieces, transport, token)
    from_chip = sent(crossing, lambda s, a, o: (s + 1 if s % 2 else s - 1, a, o))
    staying, _ = transported(False, 0, tiles, increment, multiplier, pieces, transport, token)
    from_core = sent(staying, lambda s, a, o: (s - 1 if s % 2 else s + 1, a, o))
    model_error, gradient = final(increment, base.reshape(increment.shape), from_chip, from_core)
    return (model_error[None], gradient[None], tangent[None, None])


def solution(mesh):
    in_specs = (
        P("sub", "lat", "lon", None),
        P("sub", "lat", "lon", None),
        P("sub", "lat", "lon", None),
        P("sub", ("lat", "lon"), None, None),
        P("sub", ("lat", "lon"), None),
        P("sub", None),
        P(),
        P(),
        P(),
        P(),
    )
    out_specs = (
        P("sub", "lat", "lon", None),
        P("sub", "lat", "lon", None),
        P("sub", ("lat", "lon"), None, None),
    )
    return jax.shard_map(local, mesh=mesh, in_specs=in_specs, out_specs=out_specs, check_vma=False)
```

```python
import jax
import jax.numpy as jnp
from jax import lax
from jax.experimental import pallas as pl
from jax.experimental.pallas import tpu as pltpu
from jax.sharding import PartitionSpec as P


STEPS = 4
REACH = 2 * STEPS
EDGE = REACH - 2
LANES = 128
COLS_TILE = 256
SLOTS_TILE = 512
MIRROR = (3, 2, 1, 0, 7, 6, 5, 4)
TOKEN = jax.ShapeDtypeStruct((8, LANES), jnp.float32)


CHUNK = 4


def in_hbm(*arrays):
    return [pltpu.with_memory_space_constraint(a, pltpu.HBM) for a in arrays]


def pack_kernel(inc, mul, low, high, strip, held, sems):
    lon = lax.axis_index("lon")
    rows, across = inc.shape[0], inc.shape[1]
    side = pl.multiple_of((across - REACH) * (1 - lon), REACH)
    copies = {}
    for start in range(0, rows, CHUNK):
        for f, src in enumerate((inc, mul)):
            part = pl.ds(start, CHUNK)
            copies[f, start] = pltpu.make_async_copy(src.at[part], held.at[f, part], sems.at[f, start // CHUNK])
            copies[f, start].start()
    for start in range(0, rows, CHUNK):
        for f in range(2):
            copies[f, start].wait()
            for r in range(start, start + CHUNK):
                row = held[f, r].astype(jnp.bfloat16)
                if r < REACH:
                    low[f, r] = row
                if r >= rows - REACH:
                    high[f, r - rows + REACH] = row
                strip[f, r] = held[f, r, pl.ds(side, REACH), :].astype(jnp.bfloat16)


def pack(increment, multiplier):
    rows, across, levels = increment.shape
    shapes = [(2, REACH, across), (2, REACH, across), (2, rows, REACH)]
    return pl.pallas_call(
        pack_kernel,
        in_specs=[pl.BlockSpec(memory_space=pltpu.HBM)] * 2,
        out_specs=[pl.BlockSpec(memory_space=pltpu.VMEM)] * 3,
        out_shape=[jax.ShapeDtypeStruct(s + (levels,), jnp.bfloat16) for s in shapes],
        scratch_shapes=[
            pltpu.VMEM((2,) + increment.shape, jnp.float32),
            pltpu.SemaphoreType.DMA((2, rows // CHUNK)),
        ],
        compiler_params=pltpu.CompilerParams(vmem_limit_bytes=16 << 20),
        name="pack",
    )(*in_hbm(increment, multiplier))


def corner_kernel(strip, _, low, high, token):
    rows = strip.shape[1]
    low[...] = strip[:, :EDGE]
    high[...] = strip[:, rows - EDGE :]
    token[...] = jnp.zeros_like(token)


def corners(strip, token):
    fields, _, wide, levels = strip.shape
    return pl.pallas_call(
        corner_kernel,
        in_specs=[pl.BlockSpec(memory_space=pltpu.VMEM), pl.BlockSpec(memory_space=pl.ANY)],
        out_shape=[jax.ShapeDtypeStruct((fields, EDGE, wide, levels), jnp.bfloat16)] * 2 + [TOKEN],
        compiler_params=pltpu.CompilerParams(vmem_limit_bytes=8 << 20),
        name="corners",
    )(strip, token)


def sweep(src, dst, taps, first, last, blocks):
    c0, c1, c2, c3, c4, c5, c6, c7 = taps
    group = 4
    for i in range(first, last, group):
        for b in range(blocks):
            j = 8 + 8 * b
            at = [src[i - 2 + r, j : j + 8, :] for r in range(group + 4)]
            for r in range(group):
                total = at[r + 2] + c0 * at[r]
                total = total + c1 * at[r + 1]
                total = total + c2 * at[r + 3]
                total = total + c3 * at[r + 4]
                total = total + c4 * src[i + r, j - 2 : j + 6, :]
                total = total + c5 * src[i + r, j - 1 : j + 7, :]
                total = total + c6 * src[i + r, j + 1 : j + 9, :]
                total = total + c7 * src[i + r, j + 2 : j + 10, :]
                dst[i + r, j : j + 8, :] = total


def geometry(across):
    lon = lax.axis_index("lon")
    own = pl.multiple_of(8 + REACH * lon, 8)
    beside = pl.multiple_of(8 + across * (1 - lon), 8)
    return own, beside, (across + REACH) // 8


def is_forward(crossing):
    odd = lax.rem(lax.axis_index("sub"), 2)
    return (1 - odd if crossing else odd) == 0


def place_block(forward, inc, mul, strip, bufs, sems):
    rows, across = inc.shape[0], inc.shape[1]
    own, beside, blocks = geometry(across)

    def start(src):
        for t in range(bufs.shape[0]):
            there = bufs.at[t, pl.ds(REACH, rows), pl.ds(own, across), :]
            pltpu.make_async_copy(src.at[:, :, pl.ds(t * LANES, LANES)], there, sems.at[t]).start()

    @pl.when(forward)
    def _():
        start(inc)

    @pl.when(jnp.logical_not(forward))
    def _():
        start(mul)

    f = jnp.where(forward, 0, 1)
    for t in range(bufs.shape[0]):
        for r in range(rows + 2 * REACH):
            bufs[t, r, 0:8, :] = jnp.zeros((8, LANES), jnp.float32)
            bufs[t, r, 8 * blocks + 8 : 8 * blocks + 16, :] = jnp.zeros((8, LANES), jnp.float32)
        for r in range(rows):
            lanes = slice(t * LANES, (t + 1) * LANES)
            bufs[t, REACH + r, pl.ds(beside, REACH), :] = strip[f, r, :, lanes].astype(jnp.float32)


def wait_block(inc, bufs, sems, t):
    rows, across = inc.shape[0], inc.shape[1]
    own, _, _ = geometry(across)
    there = bufs.at[t, pl.ds(REACH, rows), pl.ds(own, across), :]
    pltpu.make_async_copy(inc.at[:, :, pl.ds(0, LANES)], there, sems.at[t]).wait()


def place_halo(forward, above, below, above_corner, below_corner, bufs):
    tall, across = bufs.shape[1], above.shape[2]
    rows = tall - 2 * REACH
    own, beside, _ = geometry(across)
    f = jnp.where(forward, 0, 1)
    for t in range(bufs.shape[0]):
        lanes = slice(t * LANES, (t + 1) * LANES)
        for r in (0, 1, tall - 2, tall - 1):
            bufs[t, r, pl.ds(beside, REACH), :] = jnp.zeros((REACH, LANES), jnp.float32)
        for r in range(REACH):
            bufs[t, r, pl.ds(own, across), :] = above[f, r, :, lanes].astype(jnp.float32)
            bufs[t, rows + REACH + r, pl.ds(own, across), :] = below[f, r, :, lanes].astype(jnp.float32)
        for r in range(EDGE):
            bufs[t, REACH - EDGE + r, pl.ds(beside, REACH), :] = above_corner[f, r, :, lanes].astype(jnp.float32)
            bufs[t, rows + REACH + r, pl.ds(beside, REACH), :] = below_corner[f, r, :, lanes].astype(jnp.float32)


def taps_of(forward, rates, t):
    lanes = pl.ds(pl.multiple_of(t * LANES, LANES), LANES)
    spread = [
        jnp.broadcast_to(jnp.where(forward, rates[k : k + 1, lanes], rates[m : m + 1, lanes]), (8, LANES))
        for k, m in enumerate(MIRROR)
    ]
    rest = spread[0]
    for k in range(1, 8):
        rest = rest + spread[k]
    center = 1.0 - rest
    return [c / center for c in spread], (center * center) * (center * center)


def steps(a, b, taps, blocks, rows, ranges):
    lat, n_lat = lax.axis_index("lat"), lax.axis_size("lat")
    for spans in ranges:
        for first, last in spans:
            sweep(a, b, taps, first, last, blocks)
        low, high = spans[0][0], spans[-1][1]
        if low < REACH:

            @pl.when(lat == 0)
            def _(b=b, low=low):
                for r in range(low, REACH):
                    b[r] = jnp.zeros(b.shape[1:], jnp.float32)

            @pl.when(lat == n_lat - 1)
            def _(b=b, high=high):
                for r in range(rows + REACH, high):
                    b[r] = jnp.zeros(b.shape[1:], jnp.float32)

        a, b = b, a
    return a


def write_tile(out, done, scale, t, rows, across):
    own, _, _ = geometry(across)
    lanes = pl.ds(pl.multiple_of(t * LANES, LANES), LANES)
    for r in range(rows):
        out[r, :, lanes] = (scale[0:1] * done[REACH + r, pl.ds(own, across), :]).astype(jnp.bfloat16)


def whole_kernel(inc, mul, above, below, strip, above_corner, below_corner, rates, _, out, token, bufs, other, sems):
    rows, across = inc.shape[0], inc.shape[1]
    blocks = (across + REACH) // 8
    tall = rows + 2 * REACH
    forward = is_forward(False)
    place_block(forward, inc, mul, strip, bufs, sems)
    token[...] = jnp.zeros_like(token)
    place_halo(forward, above, below, above_corner, below_corner, bufs)
    for r in range(tall):
        other[r] = jnp.zeros(other.shape[1:], jnp.float32)
    ranges = [[(2 * k, tall - 2 * k)] for k in range(1, STEPS + 1)]

    def tile_of(t, carry):
        wait_block(inc, bufs, sems, t)
        taps, scale = taps_of(forward, rates, t)
        done = steps(bufs.at[t], other, taps, blocks, rows, ranges)
        write_tile(out, done, scale, t, rows, across)
        return carry

    lax.fori_loop(0, bufs.shape[0], tile_of, 0)


def inner_kernel(inc, mul, strip, rates, _, bufs, other, sems):
    rows, across = inc.shape[0], inc.shape[1]
    blocks = (across + REACH) // 8
    forward = is_forward(True)
    place_block(forward, inc, mul, strip, bufs, sems)
    for t in range(bufs.shape[0]):
        for r in range(rows + 2 * REACH):
            other[t, r, 0:8, :] = jnp.zeros((8, LANES), jnp.float32)
            other[t, r, 8 * blocks + 8 : 8 * blocks + 16, :] = jnp.zeros((8, LANES), jnp.float32)
    ranges = [[(REACH + 2 * k, REACH + rows - 2 * k)] for k in range(1, STEPS)]

    def tile_of(t, carry):
        wait_block(inc, bufs, sems, t)
        taps, _ = taps_of(forward, rates, t)
        steps(bufs.at[t], other.at[t], taps, blocks, rows, ranges)
        return carry

    lax.fori_loop(0, bufs.shape[0], tile_of, 0)


def outer_kernel(above, below, above_corner, below_corner, rates, _, __, out, bufs, other):
    rows, across = out.shape[0], out.shape[1]
    blocks = (across + REACH) // 8
    tall = rows + 2 * REACH
    forward = is_forward(True)
    place_halo(forward, above, below, above_corner, below_corner, bufs)
    ranges = [
        [(2 * k, REACH + 2 * k), (REACH + rows - 2 * k, tall - 2 * k)] if k < STEPS else [(2 * k, tall - 2 * k)]
        for k in range(1, STEPS + 1)
    ]

    def tile_of(t, carry):
        taps, scale = taps_of(forward, rates, t)
        done = steps(bufs.at[t], other.at[t], taps, blocks, rows, ranges)
        write_tile(out, done, scale, t, rows, across)
        return carry

    lax.fori_loop(0, bufs.shape[0], tile_of, 0)


HBM = pl.BlockSpec(memory_space=pltpu.HBM)
VMEM = pl.BlockSpec(memory_space=pltpu.VMEM)
ANY = pl.BlockSpec(memory_space=pl.ANY)


def staying_field(increment, multiplier, pieces, rates, token):
    rows, across, levels = increment.shape
    tall, wide, tiles = rows + 2 * REACH, across + REACH + 16, levels // LANES
    return pl.pallas_call(
        whole_kernel,
        in_specs=[HBM, HBM] + [VMEM] * (len(pieces) + 1) + [ANY],
        out_specs=[VMEM, VMEM],
        out_shape=[jax.ShapeDtypeStruct(increment.shape, jnp.bfloat16), TOKEN],
        scratch_shapes=[
            pltpu.VMEM((tiles, tall, wide, LANES), jnp.float32),
            pltpu.VMEM((tall, wide, LANES), jnp.float32),
            pltpu.SemaphoreType.DMA((tiles,)),
        ],
        compiler_params=pltpu.CompilerParams(vmem_limit_bytes=24 << 20),
        cost_estimate=pl.CostEstimate(flops=50_000_000, bytes_accessed=4 << 20, transcendentals=0),
        name="staying",
    )(*in_hbm(increment, multiplier), *pieces, rates, token)


def crossing_inner(increment, multiplier, strip, rates, token):
    rows, across, levels = increment.shape
    tall, wide, tiles = rows + 2 * REACH, across + REACH + 16, levels // LANES
    return pl.pallas_call(
        inner_kernel,
        in_specs=[HBM, HBM, VMEM, VMEM, ANY],
        out_specs=[VMEM] * 2,
        out_shape=[jax.ShapeDtypeStruct((tiles, tall, wide, LANES), jnp.float32)] * 2,
        scratch_shapes=[pltpu.SemaphoreType.DMA((tiles,))],
        compiler_params=pltpu.CompilerParams(vmem_limit_bytes=20 << 20),
        cost_estimate=pl.CostEstimate(flops=14_000_000, bytes_accessed=2 << 20, transcendentals=0),
        name="inner",
    )(*in_hbm(increment, multiplier), strip, rates, token)


def crossing_outer(pieces, rates, bufs, other, shape):
    above, below, _, above_corner, below_corner = pieces
    return pl.pallas_call(
        outer_kernel,
        in_specs=[VMEM] * 7,
        out_specs=[VMEM] * 3,
        out_shape=[
            jax.ShapeDtypeStruct(shape, jnp.bfloat16),
            jax.ShapeDtypeStruct(bufs.shape, jnp.float32),
            jax.ShapeDtypeStruct(other.shape, jnp.float32),
        ],
        input_output_aliases={5: 1, 6: 2},
        compiler_params=pltpu.CompilerParams(vmem_limit_bytes=20 << 20),
        cost_estimate=pl.CostEstimate(flops=36_000_000, bytes_accessed=2 << 20, transcendentals=0),
        name="outer",
    )(above, below, above_corner, below_corner, rates, bufs, other)[0]


def final_kernel(inc, base, from_chip, from_core, error_out, grad_out, error, grad, sems):
    odd = lax.rem(lax.axis_index("sub"), 2) == 1
    copies = []
    for start in range(0, inc.shape[0], CHUNK):
        for r in range(start, start + CHUNK):
            x = from_chip[r].astype(jnp.float32)
            d = from_core[r].astype(jnp.float32)
            error[r] = inc[r] - jnp.where(odd, d, x)
            grad[r] = base[r] - jnp.where(odd, x, d)
        rows = pl.ds(start, CHUNK)
        for f, (held, out) in enumerate(((error, error_out), (grad, grad_out))):
            copies.append(pltpu.make_async_copy(held.at[rows], out.at[rows], sems.at[f, start // CHUNK]))
            copies[-1].start()
    for copy in copies:
        copy.wait()


def final(increment, base, from_chip, from_core):
    hbm, vmem = pl.BlockSpec(memory_space=pltpu.HBM), pl.BlockSpec(memory_space=pltpu.VMEM)
    return pl.pallas_call(
        final_kernel,
        in_specs=[vmem] * 4,
        out_specs=[hbm] * 2,
        out_shape=[jax.ShapeDtypeStruct(increment.shape, jnp.float32)] * 2,
        scratch_shapes=[pltpu.VMEM(increment.shape, jnp.float32)] * 2
        + [pltpu.SemaphoreType.DMA((2, increment.shape[0] // CHUNK))],
        compiler_params=pltpu.CompilerParams(vmem_limit_bytes=16 << 20),
        cost_estimate=pl.CostEstimate(flops=4_000_000, bytes_accessed=10 << 20, transcendentals=0),
        name="final",
    )(increment, base, from_chip, from_core)


ROWS_BY_COLS = (((1,), (1,)), ((), ()))


def network_kernel(
    count, columns, hidden_bias, state_in, back_in, base_in, cot_in, hidden_in, output_in,
    tangents, base_out, token,
    state, back, base, cot, hidden_weight, output_weight, sems, out_sems,
):
    cols, slots = state.shape[0], cot.shape[0]
    moves = [
        (hidden_in, hidden_weight), (back_in, back), (state_in, state),
        (output_in, output_weight), (cot_in, cot), (base_in, base),
    ]
    copies = [pltpu.make_async_copy(a, b, sems.at[i]) for i, (a, b) in enumerate(moves)]
    for copy in copies:
        copy.start()
    token[...] = jnp.zeros_like(token)
    alive = lax.broadcasted_iota(jnp.int32, (1, slots), 1) < count[0]
    named = jnp.where(alive, columns[...], -1)
    outs = []
    for i, start in enumerate(range(0, cols, COLS_TILE)):
        rows = slice(start, start + COLS_TILE)
        if i == 0:
            copies[0].wait()
            copies[1].wait()
        preact = jnp.dot(back[rows], hidden_weight[...], preferred_element_type=jnp.float32) + hidden_bias[...]
        hidden = jnp.tanh(preact)
        slopes = 1.0 - hidden * hidden
        if i == 0:
            copies[2].wait()
        forward = jnp.dot(state[rows].astype(jnp.bfloat16), hidden_weight[...], preferred_element_type=jnp.float32)
        scaled = (slopes * forward).astype(jnp.bfloat16)
        if i == 0:
            copies[3].wait()
        tangent = jnp.dot(scaled, output_weight[...], preferred_element_type=jnp.float32)
        tangents[rows] = tangent.astype(jnp.bfloat16)
        ids = lax.broadcasted_iota(jnp.int32, (COLS_TILE, slots), 0) + start
        picks = jnp.where(named == ids, 1.0, 0.0).astype(jnp.bfloat16)
        if i == 0:
            copies[4].wait()
        gathered = jnp.dot(picks, cot[...], preferred_element_type=jnp.float32).astype(jnp.bfloat16)
        pulled = lax.dot_general(gathered, output_weight[...], ROWS_BY_COLS, preferred_element_type=jnp.float32)
        weighted = (slopes * pulled).astype(jnp.bfloat16)
        adjoint = lax.dot_general(weighted, hidden_weight[...], ROWS_BY_COLS, preferred_element_type=jnp.float32)
        if i == 0:
            copies[5].wait()
        base[rows] = base[rows] + adjoint
        outs.append(pltpu.make_async_copy(base.at[rows], base_out.at[rows], out_sems.at[i]))
        outs[-1].start()
    for out in outs:
        out.wait()


def network(count, columns, state, back, base, cot, hidden_weight, hidden_bias, output_weight):
    cols, levels = state.shape
    slots, chan = cot.shape
    hbm, vmem = pl.BlockSpec(memory_space=pltpu.HBM), pl.BlockSpec(memory_space=pltpu.VMEM)
    moved = (state, back, base, cot, hidden_weight, output_weight)
    return pl.pallas_call(
        network_kernel,
        in_specs=[pl.BlockSpec(memory_space=pltpu.SMEM), vmem, vmem] + [hbm] * 6,
        out_specs=[vmem, hbm, vmem],
        out_shape=[
            jax.ShapeDtypeStruct((cols, chan), jnp.bfloat16),
            jax.ShapeDtypeStruct((cols, levels), jnp.float32),
            TOKEN,
        ],
        scratch_shapes=[pltpu.VMEM(a.shape, a.dtype) for a in moved]
        + [pltpu.SemaphoreType.DMA((6,)), pltpu.SemaphoreType.DMA((cols // COLS_TILE,))],
        cost_estimate=pl.CostEstimate(
            flops=2 * (5 * cols + slots) * levels * hidden_bias.shape[1],
            bytes_accessed=12 << 20,
            transcendentals=1 << 20,
        ),
        compiler_params=pltpu.CompilerParams(vmem_limit_bytes=40 << 20),
        name="network",
    )(count, columns, hidden_bias, *in_hbm(*moved))


def spread_kernel(count, columns, tangents, _, out, held, sems):
    slots, cols = held.shape[0], tangents.shape[0]
    lane = lax.broadcasted_iota(jnp.int32, (LANES, LANES), 1)
    outs = []
    for i, start in enumerate(range(0, slots, SLOTS_TILE)):
        rows = slice(start, start + SLOTS_TILE)
        parts = []
        for s in range(start, start + SLOTS_TILE, LANES):
            alive = lax.broadcasted_iota(jnp.int32, (1, LANES), 1) + s < count[0]
            named = jnp.where(alive, columns[:, s : s + LANES], -1)
            mine = jnp.broadcast_to(named, (LANES, LANES)).T
            hits = [jnp.where(mine == lane + k, 1.0, 0.0).astype(jnp.bfloat16) for k in range(0, cols, LANES)]
            parts.append(jnp.concatenate(hits, axis=1))
        picks = jnp.concatenate(parts, axis=0)
        held[rows] = jnp.dot(picks, tangents[...], preferred_element_type=jnp.float32).astype(jnp.bfloat16)
        outs.append(pltpu.make_async_copy(held.at[rows], out.at[rows], sems.at[i]))
        outs[-1].start()
    for copy in outs:
        copy.wait()


def spread(count, columns, tangents, token):
    slots, (cols, chan) = columns.shape[1], tangents.shape
    vmem = pl.BlockSpec(memory_space=pltpu.VMEM)
    return pl.pallas_call(
        spread_kernel,
        in_specs=[pl.BlockSpec(memory_space=pltpu.SMEM), vmem, vmem, pl.BlockSpec(memory_space=pl.ANY)],
        out_specs=pl.BlockSpec(memory_space=pltpu.HBM),
        out_shape=jax.ShapeDtypeStruct((slots, chan), jnp.bfloat16),
        scratch_shapes=[
            pltpu.VMEM((slots, chan), jnp.bfloat16),
            pltpu.SemaphoreType.DMA((slots // SLOTS_TILE,)),
        ],
        compiler_params=pltpu.CompilerParams(vmem_limit_bytes=24 << 20),
        cost_estimate=pl.CostEstimate(flops=2 * slots * cols * chan, bytes_accessed=4 << 20, transcendentals=0),
        name="spread",
    )(count, columns, tangents, token)


def sent(array, to):
    counts = [lax.axis_size(axis) for axis in ("sub", "lat", "lon")]
    flat = lambda s, a, o: (s * counts[1] + a) * counts[2] + o
    pairs = []
    for s in range(counts[0]):
        for a in range(counts[1]):
            for o in range(counts[2]):
                target = to(s, a, o)
                if all(0 <= t < n for t, n in zip(target, counts)):
                    pairs.append((flat(s, a, o), flat(*target)))
    return lax.ppermute(array, ("sub", "lat", "lon"), pairs)


def local(
    increment,
    multiplier,
    background,
    obs_cotangent,
    obs_column,
    obs_count,
    transport,
    hidden_weight,
    hidden_bias,
    output_weight,
):
    increment, multiplier = increment[0], multiplier[0]
    levels = increment.shape[2]
    low, high, strip = pack(increment, multiplier)
    above = sent(high, lambda s, a, o: (s, a + 1, o))
    below = sent(low, lambda s, a, o: (s, a - 1, o))
    across = sent(strip, lambda s, a, o: (s, a, 1 - o))
    myself = lax.axis_index(("lat", "lon"))
    my_count = lax.dynamic_slice(obs_count[0], (myself,), (1,))
    tangents, base, token = network(
        my_count,
        obs_column[0],
        increment.reshape(-1, levels),
        background[0].reshape(-1, levels),
        multiplier.reshape(-1, levels),
        obs_cotangent[0, 0],
        hidden_weight,
        hidden_bias[None, :],
        output_weight,
    )
    low_corner, high_corner, token = corners(across, token)
    above_corner = sent(high_corner, lambda s, a, o: (s, a + 1, o))
    below_corner = sent(low_corner, lambda s, a, o: (s, a - 1, o))
    pieces = [above, below, across, above_corner, below_corner]
    pieces = [above, below, across, above_corner, below_corner]
    bufs, other = crossing_inner(increment, multiplier, across, transport, token)
    crossing = crossing_outer(pieces, transport, bufs, other, increment.shape)
    from_chip = sent(crossing, lambda s, a, o: (s + 1 if s % 2 else s - 1, a, o))
    staying, token = staying_field(increment, multiplier, pieces, transport, token)
    from_core = sent(staying, lambda s, a, o: (s - 1 if s % 2 else s + 1, a, o))
    tangent = spread(my_count, obs_column[0], tangents, token)
    model_error, gradient = final(increment, base.reshape(increment.shape), from_chip, from_core)
    return (model_error[None], gradient[None], tangent[None, None])


def solution(mesh):
    in_specs = (
        P("sub", "lat", "lon", None),
        P("sub", "lat", "lon", None),
        P("sub", "lat", "lon", None),
        P("sub", ("lat", "lon"), None, None),
        P("sub", ("lat", "lon"), None),
        P("sub", None),
        P(),
        P(),
        P(),
        P(),
    )
    out_specs = (
        P("sub", "lat", "lon", None),
        P("sub", "lat", "lon", None),
        P("sub", ("lat", "lon"), None, None),
    )
    return jax.shard_map(local, mesh=mesh, in_specs=in_specs, out_specs=out_specs, check_vma=False)
```

```python
import jax
import jax.numpy as jnp
from jax import lax
from jax.experimental import pallas as pl
from jax.experimental.pallas import tpu as pltpu
from jax.sharding import PartitionSpec as P


STEPS = 4
REACH = 2 * STEPS
EDGE = REACH - 2
LANES = 128
COLS_TILE = 256
SLOTS_TILE = 512
MIRROR = (3, 2, 1, 0, 7, 6, 5, 4)
TOKEN = jax.ShapeDtypeStruct((8, LANES), jnp.float32)


CHUNK = 4


def is_even_lat():
    return lax.rem(lax.axis_index("lat"), 2) == 0


def in_hbm(*arrays):
    return [pltpu.with_memory_space_constraint(a, pltpu.HBM) for a in arrays]


def pack_kernel(inc, mul, near, far, strip, held, sems):
    lon = lax.axis_index("lon")
    rows, across = inc.shape[0], inc.shape[1]
    side = pl.multiple_of((across - REACH) * (1 - lon), REACH)
    copies = {}
    for start in range(0, rows, CHUNK):
        for f, src in enumerate((inc, mul)):
            part = pl.ds(start, CHUNK)
            copies[f, start] = pltpu.make_async_copy(src.at[part], held.at[f, part], sems.at[f, start // CHUNK])
            copies[f, start].start()
    for start in range(0, rows, CHUNK):
        for f in range(2):
            copies[f, start].wait()
            for r in range(start, start + CHUNK):
                strip[f, r] = held[f, r, pl.ds(side, REACH), :].astype(jnp.bfloat16)

    even = is_even_lat()

    def split(low, high):
        for f in range(2):
            for r in range(REACH):
                low[f, r] = held[f, r].astype(jnp.bfloat16)
                high[f, r] = held[f, rows - REACH + r].astype(jnp.bfloat16)

    pl.when(even)(lambda: split(far, near))
    pl.when(jnp.logical_not(even))(lambda: split(near, far))


def pack(increment, multiplier):
    rows, across, levels = increment.shape
    shapes = [(2, REACH, across), (2, REACH, across), (2, rows, REACH)]
    return pl.pallas_call(
        pack_kernel,
        in_specs=[pl.BlockSpec(memory_space=pltpu.HBM)] * 2,
        out_specs=[pl.BlockSpec(memory_space=pltpu.VMEM)] * 3,
        out_shape=[jax.ShapeDtypeStruct(s + (levels,), jnp.bfloat16) for s in shapes],
        scratch_shapes=[
            pltpu.VMEM((2,) + increment.shape, jnp.float32),
            pltpu.SemaphoreType.DMA((2, rows // CHUNK)),
        ],
        compiler_params=pltpu.CompilerParams(vmem_limit_bytes=16 << 20),
        name="pack",
    )(*in_hbm(increment, multiplier))


def corner_kernel(strip, _, near, far, token):
    rows = strip.shape[1]
    even = is_even_lat()

    def split(low, high):
        low[...] = strip[:, :EDGE]
        high[...] = strip[:, rows - EDGE :]

    pl.when(even)(lambda: split(far, near))
    pl.when(jnp.logical_not(even))(lambda: split(near, far))
    token[...] = jnp.zeros_like(token)


def corners(strip, token):
    fields, _, wide, levels = strip.shape
    return pl.pallas_call(
        corner_kernel,
        in_specs=[pl.BlockSpec(memory_space=pltpu.VMEM), pl.BlockSpec(memory_space=pl.ANY)],
        out_shape=[jax.ShapeDtypeStruct((fields, EDGE, wide, levels), jnp.bfloat16)] * 2 + [TOKEN],
        compiler_params=pltpu.CompilerParams(vmem_limit_bytes=8 << 20),
        name="corners",
    )(strip, token)


def sweep(src, dst, taps, first, last, blocks):
    c0, c1, c2, c3, c4, c5, c6, c7 = taps
    group = 4
    for i in range(first, last, group):
        for b in range(blocks):
            j = 8 + 8 * b
            at = [src[i - 2 + r, j : j + 8, :] for r in range(group + 4)]
            for r in range(group):
                total = at[r + 2] + c0 * at[r]
                total = total + c1 * at[r + 1]
                total = total + c2 * at[r + 3]
                total = total + c3 * at[r + 4]
                total = total + c4 * src[i + r, j - 2 : j + 6, :]
                total = total + c5 * src[i + r, j - 1 : j + 7, :]
                total = total + c6 * src[i + r, j + 1 : j + 9, :]
                total = total + c7 * src[i + r, j + 2 : j + 10, :]
                dst[i + r, j : j + 8, :] = total


def geometry(across):
    lon = lax.axis_index("lon")
    own = pl.multiple_of(8 + REACH * lon, 8)
    beside = pl.multiple_of(8 + across * (1 - lon), 8)
    return own, beside, (across + REACH) // 8


def is_forward(crossing):
    odd = lax.rem(lax.axis_index("sub"), 2)
    return (1 - odd if crossing else odd) == 0


def place_block(forward, inc, mul, strip, bufs, sems):
    rows, across = inc.shape[0], inc.shape[1]
    own, beside, blocks = geometry(across)

    def start(src):
        for t in range(bufs.shape[0]):
            there = bufs.at[t, pl.ds(REACH, rows), pl.ds(own, across), :]
            pltpu.make_async_copy(src.at[:, :, pl.ds(t * LANES, LANES)], there, sems.at[t]).start()

    @pl.when(forward)
    def _():
        start(inc)

    @pl.when(jnp.logical_not(forward))
    def _():
        start(mul)

    f = jnp.where(forward, 0, 1)
    for t in range(bufs.shape[0]):
        for r in range(rows + 2 * REACH):
            bufs[t, r, 0:8, :] = jnp.zeros((8, LANES), jnp.float32)
            bufs[t, r, 8 * blocks + 8 : 8 * blocks + 16, :] = jnp.zeros((8, LANES), jnp.float32)
        for r in range(rows):
            lanes = slice(t * LANES, (t + 1) * LANES)
            bufs[t, REACH + r, pl.ds(beside, REACH), :] = strip[f, r, :, lanes].astype(jnp.float32)


def wait_block(inc, bufs, sems, t):
    rows, across = inc.shape[0], inc.shape[1]
    own, _, _ = geometry(across)
    there = bufs.at[t, pl.ds(REACH, rows), pl.ds(own, across), :]
    pltpu.make_async_copy(inc.at[:, :, pl.ds(0, LANES)], there, sems.at[t]).wait()


def place_halo(forward, near, far, near_corner, far_corner, bufs):
    tall, across = bufs.shape[1], near.shape[2]
    rows = tall - 2 * REACH
    own, beside, _ = geometry(across)
    f = jnp.where(forward, 0, 1)
    even = is_even_lat()
    near_row, far_row = (jnp.where(e, rows + REACH, 0) for e in (even, jnp.logical_not(even)))
    skip = REACH - EDGE
    near_edge, far_edge = (jnp.where(e, rows + REACH, skip) for e in (even, jnp.logical_not(even)))
    for t in range(bufs.shape[0]):
        lanes = slice(t * LANES, (t + 1) * LANES)
        for r in (0, 1, tall - 2, tall - 1):
            bufs[t, r, pl.ds(beside, REACH), :] = jnp.zeros((REACH, LANES), jnp.float32)
        for r in range(REACH):
            bufs[t, near_row + r, pl.ds(own, across), :] = near[f, r, :, lanes].astype(jnp.float32)
            bufs[t, far_row + r, pl.ds(own, across), :] = far[f, r, :, lanes].astype(jnp.float32)
        for r in range(EDGE):
            bufs[t, near_edge + r, pl.ds(beside, REACH), :] = near_corner[f, r, :, lanes].astype(jnp.float32)
            bufs[t, far_edge + r, pl.ds(beside, REACH), :] = far_corner[f, r, :, lanes].astype(jnp.float32)


def taps_of(forward, rates, t):
    lanes = pl.ds(pl.multiple_of(t * LANES, LANES), LANES)
    spread = [
        jnp.broadcast_to(jnp.where(forward, rates[k : k + 1, lanes], rates[m : m + 1, lanes]), (8, LANES))
        for k, m in enumerate(MIRROR)
    ]
    rest = spread[0]
    for k in range(1, 8):
        rest = rest + spread[k]
    center = 1.0 - rest
    return [c / center for c in spread], (center * center) * (center * center)


def steps(a, b, taps, blocks, rows, ranges):
    lat, n_lat = lax.axis_index("lat"), lax.axis_size("lat")
    for spans in ranges:
        for first, last in spans:
            sweep(a, b, taps, first, last, blocks)
        low, high = spans[0][0], spans[-1][1]
        if low < REACH:

            @pl.when(lat == 0)
            def _(b=b, low=low):
                for r in range(low, REACH):
                    b[r] = jnp.zeros(b.shape[1:], jnp.float32)

            @pl.when(lat == n_lat - 1)
            def _(b=b, high=high):
                for r in range(rows + REACH, high):
                    b[r] = jnp.zeros(b.shape[1:], jnp.float32)

        a, b = b, a
    return a


def write_tile(out, done, scale, t, rows, across):
    own, _, _ = geometry(across)
    lanes = pl.ds(pl.multiple_of(t * LANES, LANES), LANES)
    for r in range(rows):
        out[r, :, lanes] = (scale[0:1] * done[REACH + r, pl.ds(own, across), :]).astype(jnp.bfloat16)


def whole_kernel(inc, mul, near, far, strip, near_corner, far_corner, rates, _, out, token, bufs, other, sems):
    rows, across = inc.shape[0], inc.shape[1]
    blocks = (across + REACH) // 8
    tall = rows + 2 * REACH
    forward = is_forward(False)
    place_block(forward, inc, mul, strip, bufs, sems)
    token[...] = jnp.zeros_like(token)
    place_halo(forward, near, far, near_corner, far_corner, bufs)
    for r in range(tall):
        other[r] = jnp.zeros(other.shape[1:], jnp.float32)
    ranges = [[(2 * k, tall - 2 * k)] for k in range(1, STEPS + 1)]

    def tile_of(t, carry):
        wait_block(inc, bufs, sems, t)
        taps, scale = taps_of(forward, rates, t)
        done = steps(bufs.at[t], other, taps, blocks, rows, ranges)
        write_tile(out, done, scale, t, rows, across)
        return carry

    lax.fori_loop(0, bufs.shape[0], tile_of, 0)


def inner_kernel(inc, mul, strip, rates, _, bufs, other, sems):
    rows, across = inc.shape[0], inc.shape[1]
    blocks = (across + REACH) // 8
    forward = is_forward(True)
    place_block(forward, inc, mul, strip, bufs, sems)
    for t in range(bufs.shape[0]):
        for r in range(rows + 2 * REACH):
            other[t, r, 0:8, :] = jnp.zeros((8, LANES), jnp.float32)
            other[t, r, 8 * blocks + 8 : 8 * blocks + 16, :] = jnp.zeros((8, LANES), jnp.float32)
    ranges = [[(REACH + 2 * k, REACH + rows - 2 * k)] for k in range(1, STEPS)]

    def tile_of(t, carry):
        wait_block(inc, bufs, sems, t)
        taps, _ = taps_of(forward, rates, t)
        steps(bufs.at[t], other.at[t], taps, blocks, rows, ranges)
        return carry

    lax.fori_loop(0, bufs.shape[0], tile_of, 0)


def outer_kernel(near, far, near_corner, far_corner, rates, _, __, out, bufs, other):
    rows, across = out.shape[0], out.shape[1]
    blocks = (across + REACH) // 8
    tall = rows + 2 * REACH
    forward = is_forward(True)
    place_halo(forward, near, far, near_corner, far_corner, bufs)
    ranges = [
        [(2 * k, REACH + 2 * k), (REACH + rows - 2 * k, tall - 2 * k)] if k < STEPS else [(2 * k, tall - 2 * k)]
        for k in range(1, STEPS + 1)
    ]

    def tile_of(t, carry):
        taps, scale = taps_of(forward, rates, t)
        done = steps(bufs.at[t], other.at[t], taps, blocks, rows, ranges)
        write_tile(out, done, scale, t, rows, across)
        return carry

    lax.fori_loop(0, bufs.shape[0], tile_of, 0)


HBM = pl.BlockSpec(memory_space=pltpu.HBM)
VMEM = pl.BlockSpec(memory_space=pltpu.VMEM)
ANY = pl.BlockSpec(memory_space=pl.ANY)


def staying_field(increment, multiplier, pieces, rates, token):
    rows, across, levels = increment.shape
    tall, wide, tiles = rows + 2 * REACH, across + REACH + 16, levels // LANES
    return pl.pallas_call(
        whole_kernel,
        in_specs=[HBM, HBM] + [VMEM] * (len(pieces) + 1) + [ANY],
        out_specs=[VMEM, VMEM],
        out_shape=[jax.ShapeDtypeStruct(increment.shape, jnp.bfloat16), TOKEN],
        scratch_shapes=[
            pltpu.VMEM((tiles, tall, wide, LANES), jnp.float32),
            pltpu.VMEM((tall, wide, LANES), jnp.float32),
            pltpu.SemaphoreType.DMA((tiles,)),
        ],
        compiler_params=pltpu.CompilerParams(vmem_limit_bytes=24 << 20),
        cost_estimate=pl.CostEstimate(flops=50_000_000, bytes_accessed=4 << 20, transcendentals=0),
        name="staying",
    )(*in_hbm(increment, multiplier), *pieces, rates, token)


def crossing_inner(increment, multiplier, strip, rates, token):
    rows, across, levels = increment.shape
    tall, wide, tiles = rows + 2 * REACH, across + REACH + 16, levels // LANES
    return pl.pallas_call(
        inner_kernel,
        in_specs=[HBM, HBM, VMEM, VMEM, ANY],
        out_specs=[VMEM] * 2,
        out_shape=[jax.ShapeDtypeStruct((tiles, tall, wide, LANES), jnp.float32)] * 2,
        scratch_shapes=[pltpu.SemaphoreType.DMA((tiles,))],
        compiler_params=pltpu.CompilerParams(vmem_limit_bytes=20 << 20),
        cost_estimate=pl.CostEstimate(flops=14_000_000, bytes_accessed=2 << 20, transcendentals=0),
        name="inner",
    )(*in_hbm(increment, multiplier), strip, rates, token)


def crossing_outer(pieces, rates, bufs, other, shape):
    near, far, _, near_corner, far_corner = pieces
    return pl.pallas_call(
        outer_kernel,
        in_specs=[VMEM] * 7,
        out_specs=[VMEM] * 3,
        out_shape=[
            jax.ShapeDtypeStruct(shape, jnp.bfloat16),
            jax.ShapeDtypeStruct(bufs.shape, jnp.float32),
            jax.ShapeDtypeStruct(other.shape, jnp.float32),
        ],
        input_output_aliases={5: 1, 6: 2},
        compiler_params=pltpu.CompilerParams(vmem_limit_bytes=20 << 20),
        cost_estimate=pl.CostEstimate(flops=36_000_000, bytes_accessed=2 << 20, transcendentals=0),
        name="outer",
    )(near, far, near_corner, far_corner, rates, bufs, other)[0]


def final_kernel(inc, base, from_chip, from_core, error_out, grad_out, error, grad, sems):
    odd = lax.rem(lax.axis_index("sub"), 2) == 1
    copies = []
    for start in range(0, inc.shape[0], CHUNK):
        for r in range(start, start + CHUNK):
            x = from_chip[r].astype(jnp.float32)
            d = from_core[r].astype(jnp.float32)
            error[r] = inc[r] - jnp.where(odd, d, x)
            grad[r] = base[r] - jnp.where(odd, x, d)
        rows = pl.ds(start, CHUNK)
        for f, (held, out) in enumerate(((error, error_out), (grad, grad_out))):
            copies.append(pltpu.make_async_copy(held.at[rows], out.at[rows], sems.at[f, start // CHUNK]))
            copies[-1].start()
    for copy in copies:
        copy.wait()


def final(increment, base, from_chip, from_core):
    hbm, vmem = pl.BlockSpec(memory_space=pltpu.HBM), pl.BlockSpec(memory_space=pltpu.VMEM)
    return pl.pallas_call(
        final_kernel,
        in_specs=[vmem] * 4,
        out_specs=[hbm] * 2,
        out_shape=[jax.ShapeDtypeStruct(increment.shape, jnp.float32)] * 2,
        scratch_shapes=[pltpu.VMEM(increment.shape, jnp.float32)] * 2
        + [pltpu.SemaphoreType.DMA((2, increment.shape[0] // CHUNK))],
        compiler_params=pltpu.CompilerParams(vmem_limit_bytes=16 << 20),
        cost_estimate=pl.CostEstimate(flops=4_000_000, bytes_accessed=10 << 20, transcendentals=0),
        name="final",
    )(increment, base, from_chip, from_core)


ROWS_BY_COLS = (((1,), (1,)), ((), ()))


def network_kernel(
    count, columns, hidden_bias, state_in, back_in, base_in, cot_in, hidden_in, output_in,
    tangents, base_out, token,
    state, back, base, cot, hidden_weight, output_weight, sems, out_sems,
):
    cols, slots = state.shape[0], cot.shape[0]
    moves = [
        (hidden_in, hidden_weight), (back_in, back), (state_in, state),
        (output_in, output_weight), (cot_in, cot), (base_in, base),
    ]
    copies = [pltpu.make_async_copy(a, b, sems.at[i]) for i, (a, b) in enumerate(moves)]
    for copy in copies:
        copy.start()
    token[...] = jnp.zeros_like(token)
    alive = lax.broadcasted_iota(jnp.int32, (1, slots), 1) < count[0]
    named = jnp.where(alive, columns[...], -1)
    outs = []
    for i, start in enumerate(range(0, cols, COLS_TILE)):
        rows = slice(start, start + COLS_TILE)
        if i == 0:
            copies[0].wait()
            copies[1].wait()
        preact = jnp.dot(back[rows], hidden_weight[...], preferred_element_type=jnp.float32) + hidden_bias[...]
        hidden = jnp.tanh(preact)
        slopes = 1.0 - hidden * hidden
        if i == 0:
            copies[2].wait()
        forward = jnp.dot(state[rows].astype(jnp.bfloat16), hidden_weight[...], preferred_element_type=jnp.float32)
        scaled = (slopes * forward).astype(jnp.bfloat16)
        if i == 0:
            copies[3].wait()
        tangent = jnp.dot(scaled, output_weight[...], preferred_element_type=jnp.float32)
        tangents[rows] = tangent.astype(jnp.bfloat16)
        ids = lax.broadcasted_iota(jnp.int32, (COLS_TILE, slots), 0) + start
        picks = jnp.where(named == ids, 1.0, 0.0).astype(jnp.bfloat16)
        if i == 0:
            copies[4].wait()
        gathered = jnp.dot(picks, cot[...], preferred_element_type=jnp.float32).astype(jnp.bfloat16)
        pulled = lax.dot_general(gathered, output_weight[...], ROWS_BY_COLS, preferred_element_type=jnp.float32)
        weighted = (slopes * pulled).astype(jnp.bfloat16)
        adjoint = lax.dot_general(weighted, hidden_weight[...], ROWS_BY_COLS, preferred_element_type=jnp.float32)
        if i == 0:
            copies[5].wait()
        base[rows] = base[rows] + adjoint
        outs.append(pltpu.make_async_copy(base.at[rows], base_out.at[rows], out_sems.at[i]))
        outs[-1].start()
    for out in outs:
        out.wait()


def network(count, columns, state, back, base, cot, hidden_weight, hidden_bias, output_weight):
    cols, levels = state.shape
    slots, chan = cot.shape
    hbm, vmem = pl.BlockSpec(memory_space=pltpu.HBM), pl.BlockSpec(memory_space=pltpu.VMEM)
    moved = (state, back, base, cot, hidden_weight, output_weight)
    return pl.pallas_call(
        network_kernel,
        in_specs=[pl.BlockSpec(memory_space=pltpu.SMEM), vmem, vmem] + [hbm] * 6,
        out_specs=[vmem, hbm, vmem],
        out_shape=[
            jax.ShapeDtypeStruct((cols, chan), jnp.bfloat16),
            jax.ShapeDtypeStruct((cols, levels), jnp.float32),
            TOKEN,
        ],
        scratch_shapes=[pltpu.VMEM(a.shape, a.dtype) for a in moved]
        + [pltpu.SemaphoreType.DMA((6,)), pltpu.SemaphoreType.DMA((cols // COLS_TILE,))],
        cost_estimate=pl.CostEstimate(
            flops=2 * (5 * cols + slots) * levels * hidden_bias.shape[1],
            bytes_accessed=12 << 20,
            transcendentals=1 << 20,
        ),
        compiler_params=pltpu.CompilerParams(vmem_limit_bytes=40 << 20),
        name="network",
    )(count, columns, hidden_bias, *in_hbm(*moved))


def spread_kernel(count, columns, tangents, _, out, held, sems):
    slots, cols = held.shape[0], tangents.shape[0]
    lane = lax.broadcasted_iota(jnp.int32, (LANES, LANES), 1)
    outs = []
    for i, start in enumerate(range(0, slots, SLOTS_TILE)):
        rows = slice(start, start + SLOTS_TILE)
        parts = []
        for s in range(start, start + SLOTS_TILE, LANES):
            alive = lax.broadcasted_iota(jnp.int32, (1, LANES), 1) + s < count[0]
            named = jnp.where(alive, columns[:, s : s + LANES], -1)
            mine = jnp.broadcast_to(named, (LANES, LANES)).T
            hits = [jnp.where(mine == lane + k, 1.0, 0.0).astype(jnp.bfloat16) for k in range(0, cols, LANES)]
            parts.append(jnp.concatenate(hits, axis=1))
        picks = jnp.concatenate(parts, axis=0)
        held[rows] = jnp.dot(picks, tangents[...], preferred_element_type=jnp.float32).astype(jnp.bfloat16)
        outs.append(pltpu.make_async_copy(held.at[rows], out.at[rows], sems.at[i]))
        outs[-1].start()
    for copy in outs:
        copy.wait()


def spread(count, columns, tangents, token):
    slots, (cols, chan) = columns.shape[1], tangents.shape
    vmem = pl.BlockSpec(memory_space=pltpu.VMEM)
    return pl.pallas_call(
        spread_kernel,
        in_specs=[pl.BlockSpec(memory_space=pltpu.SMEM), vmem, vmem, pl.BlockSpec(memory_space=pl.ANY)],
        out_specs=pl.BlockSpec(memory_space=pltpu.HBM),
        out_shape=jax.ShapeDtypeStruct((slots, chan), jnp.bfloat16),
        scratch_shapes=[
            pltpu.VMEM((slots, chan), jnp.bfloat16),
            pltpu.SemaphoreType.DMA((slots // SLOTS_TILE,)),
        ],
        compiler_params=pltpu.CompilerParams(vmem_limit_bytes=24 << 20),
        cost_estimate=pl.CostEstimate(flops=2 * slots * cols * chan, bytes_accessed=4 << 20, transcendentals=0),
        name="spread",
    )(count, columns, tangents, token)


def sent(array, to):
    counts = [lax.axis_size(axis) for axis in ("sub", "lat", "lon")]
    flat = lambda s, a, o: (s * counts[1] + a) * counts[2] + o
    pairs = []
    for s in range(counts[0]):
        for a in range(counts[1]):
            for o in range(counts[2]):
                target = to(s, a, o)
                if all(0 <= t < n for t, n in zip(target, counts)):
                    pairs.append((flat(s, a, o), flat(*target)))
    return lax.ppermute(array, ("sub", "lat", "lon"), pairs)


def local(
    increment,
    multiplier,
    background,
    obs_cotangent,
    obs_column,
    obs_count,
    transport,
    hidden_weight,
    hidden_bias,
    output_weight,
):
    increment, multiplier = increment[0], multiplier[0]
    levels = increment.shape[2]
    near_out, far_out, strip = pack(increment, multiplier)
    partner = lambda s, a, o: (s, a - 1 if a % 2 else a + 1, o)
    other_side = lambda s, a, o: (s, a + 1 if a % 2 else a - 1, o)
    near = sent(near_out, partner)
    far = sent(far_out, other_side)
    across = sent(strip, lambda s, a, o: (s, a, 1 - o))
    myself = lax.axis_index(("lat", "lon"))
    my_count = lax.dynamic_slice(obs_count[0], (myself,), (1,))
    tangents, base, token = network(
        my_count,
        obs_column[0],
        increment.reshape(-1, levels),
        background[0].reshape(-1, levels),
        multiplier.reshape(-1, levels),
        obs_cotangent[0, 0],
        hidden_weight,
        hidden_bias[None, :],
        output_weight,
    )
    near_corner, far_corner, token = corners(across, token)
    near_corner = sent(near_corner, partner)
    far_corner = sent(far_corner, other_side)
    pieces = [near, far, across, near_corner, far_corner]
    bufs, other = crossing_inner(increment, multiplier, across, transport, token)
    crossing = crossing_outer(pieces, transport, bufs, other, increment.shape)
    from_chip = sent(crossing, lambda s, a, o: (s + 1 if s % 2 else s - 1, a, o))
    staying, token = staying_field(increment, multiplier, pieces, transport, token)
    from_core = sent(staying, lambda s, a, o: (s - 1 if s % 2 else s + 1, a, o))
    tangent = spread(my_count, obs_column[0], tangents, token)
    model_error, gradient = final(increment, base.reshape(increment.shape), from_chip, from_core)
    return (model_error[None], gradient[None], tangent[None, None])


def solution(mesh):
    in_specs = (
        P("sub", "lat", "lon", None),
        P("sub", "lat", "lon", None),
        P("sub", "lat", "lon", None),
        P("sub", ("lat", "lon"), None, None),
        P("sub", ("lat", "lon"), None),
        P("sub", None),
        P(),
        P(),
        P(),
        P(),
    )
    out_specs = (
        P("sub", "lat", "lon", None),
        P("sub", "lat", "lon", None),
        P("sub", ("lat", "lon"), None, None),
    )
    return jax.shard_map(local, mesh=mesh, in_specs=in_specs, out_specs=out_specs, check_vma=False)
```
